32 devices in a mesh: section: 2 (over core), dp: 4 (over z), tensor: 4 (over y, x).
Axes of the slice: x: 2, y: 2, z: 4, core: 2. Of those that a mesh axis runs over, the one named last changes fastest.
Arguments:
- block_input: bfloat16 [4, 512, 2048], P(None, 'dp'), may hold values from -6 to 6
- cotangent: bfloat16 [4, 512, 2048], P(None, 'dp'), may hold values from -6 to 6
- segments: int32 [4, 512], P(None, 'dp'), may hold values from -1 to 127, as said below
- ln_gain: float32 [2, 2048], P('section'), may hold values from 0.5 to 1.5
- ln_bias: float32 [2, 2048], P('section'), may hold values from -3 to 3
- qkv_weight: bfloat16 [2, 3, 2048, 2048], P('section', None, None, 'tensor')
- qv_bias: float32 [2, 2, 2048], P('section', None, 'tensor'), may hold values from -3 to 3
- dense_weight: bfloat16 [2, 2048, 2048], P('section', 'tensor'), may hold values from -0.75 to 0.75
- out_bias: float32 [2, 2048], P('section'), may hold values from -3 to 3
- fc1_weight: bfloat16 [2, 2048, 8192], P('section', None, 'tensor'), may hold values from -0.125 to 0.125
- fc1_bias: float32 [2, 8192], P('section', 'tensor'), may hold values from -3 to 3
- fc2_weight: bfloat16 [2, 8192, 2048], P('section', 'tensor'), may hold values from -0.0625 to 0.0625
Outputs:
- layer_out: bfloat16 [2, 4, 512, 2048], P('section', None, ('dp', 'tensor'))
- in_grad: bfloat16 [2, 4, 512, 2048], P('section', None, ('dp', 'tensor'))
- grad_ln_gain: float32 [2, 2048], P('section')
- grad_ln_bias: float32 [2, 2048], P('section')
- grad_qkv: float32 [2, 3, 2048, 2048], P('section', None, 'dp', 'tensor')
- grad_qv_bias: float32 [2, 2, 2048], P('section', None, 'tensor')
- grad_dense: float32 [2, 2048, 2048], P('section', 'tensor', 'dp')
- grad_out_bias: float32 [2, 2048], P('section')
- grad_fc1: float32 [2, 2048, 8192], P('section', 'dp', 'tensor')
- grad_fc1_bias: float32 [2, 8192], P('section', 'tensor')
- grad_fc2: float32 [2, 8192, 2048], P('section', 'tensor', 'dp')
The draws below stay inside these ranges and needn't reach their ends.
Inputs may be any that keep to these rules, and one draw needn't show every extreme that they name: `segments`: within each data group's 128 positions of a micro-batch the ids start at 0 and never fall over a first stretch of 64 or more positions, after which the rest are -1 for padding. In every draw the first micro-batch of the first data group has no padding and gives each position a sequence of its own, and the last one of the last data group has exactly 64 live positions.
All inputs are finite; a program needn't handle non-finite values.
Results may differ from the reference program's by a relative error of at most 0.014.
Values may be sent and summed in bfloat16 or wider, within the bound.
A program may use at most 320 MiB of HBM per device.

```python
import jax
import jax.numpy as jnp
from jax import lax

D = 2048
HEAD_DIM = 64
ROT = 32
FF = 8192
M = 4
MB = 128
TOKENS = 512
N_DP = 4


def draw_segments(key, part):
    key_live, key_edge = jax.random.split(jax.random.fold_in(key, 11), 2)
    live_count = jax.random.randint(key_live, (M, N_DP, 1), MB // 2, MB + 1)
    block_row = jnp.arange(M, dtype=jnp.int32)[:, None, None]
    block_col = jnp.arange(N_DP, dtype=jnp.int32)[None, :, None]
    first_block = (block_row == 0) & (block_col == 0)
    live_count = jnp.where(first_block, MB, live_count)
    live_count = jnp.where((block_row == M - 1) & (block_col == N_DP - 1), MB // 2, live_count)
    position = jnp.arange(MB, dtype=jnp.int32)[None, None, :]
    edges = (jax.random.randint(key_edge, (M, N_DP, MB), 0, max(MB // 4, 2)) == 0).astype(jnp.int32)
    edges = jnp.where(first_block, 1, edges)
    edges = jnp.where(position > 0, edges, 0)
    ids = jnp.cumsum(edges, axis=2).astype(jnp.int32)
    result = jnp.where(position < live_count, ids, -1).astype(jnp.int32)
    return result.reshape(M, N_DP * MB)


def draw_qkv_weight(key, part):
    key_one = jax.random.fold_in(jax.random.fold_in(key, 23), 0)
    base = jax.random.normal(key_one, (2, 3, D, D), jnp.float32) * D ** (-0.5)
    return base.astype(jnp.bfloat16)


def shard_levels(own_key, extent, cuts, low, largest):
    loudness = 1.0
    for axis_at, parts in cuts:
        heights = jax.random.uniform(jax.random.fold_in(jax.random.fold_in(own_key, 6), axis_at), (parts,), jnp.float32, low / len(cuts), largest / len(cuts))
        loudness = loudness * jnp.repeat(jnp.exp(heights), extent[axis_at] // parts).reshape((-1,) + (1,) * (len(extent) - 1 - axis_at))
    return loudness


def bell_draw(rng, extent, width, bound, pieces=(), kind=jnp.bfloat16):
    values = jax.random.normal(rng, extent, jnp.float32) * width
    if len(pieces) > 0:
        values = shard_levels(rng, extent, pieces, -0.22, 0.18) * values
    return jnp.clip(values, min=-bound, max=bound).astype(kind)


def setup_inputs(seed: int = 0) -> dict:
    arg_keys = jax.random.split(jax.random.key(seed), 13)
    block_input = bell_draw(arg_keys[0], (M, TOKENS, D), 1.0, 6.0, ((1, 4),))
    cotangent = bell_draw(arg_keys[1], (M, TOKENS, D), 1.0, 6.0, ((1, 4),))
    segments = draw_segments(jax.random.fold_in(arg_keys[12], 71), 0)
    ln_gain = jnp.clip(1.0 + 0.1 * jax.random.normal(arg_keys[3], (2, D), jnp.float32), 0.5, 1.5)
    ln_bias = bell_draw(arg_keys[4], (2, D), 0.5, 3.0, ((0, 2),), jnp.float32)
    qkv_weight = draw_qkv_weight(jax.random.fold_in(arg_keys[12], 71), 0)
    qv_bias = bell_draw(arg_keys[6], (2, 2, D), 0.5, 3.0, ((0, 2), (2, 4)), jnp.float32)
    dense_weight = bell_draw(arg_keys[7], (2, D, D), (D // 32) ** -0.5, 0.75, ((0, 2), (1, 4)))
    out_bias = bell_draw(arg_keys[8], (2, D), 0.5, 3.0, ((0, 2),), jnp.float32)
    fc1_weight = bell_draw(arg_keys[9], (2, D, FF), D ** -0.5, 0.125, ((0, 2), (2, 4)))
    fc1_bias = bell_draw(arg_keys[10], (2, FF), 0.5, 3.0, ((0, 2), (1, 4)), jnp.float32)
    fc2_weight = bell_draw(arg_keys[11], (2, FF, D), FF ** -0.5, 0.0625, ((0, 2), (1, 4)))
    return dict(block_input=block_input, cotangent=cotangent, segments=segments, ln_gain=ln_gain, ln_bias=ln_bias, qkv_weight=qkv_weight, qv_bias=qv_bias, dense_weight=dense_weight, out_bias=out_bias, fc1_weight=fc1_weight, fc1_bias=fc1_bias, fc2_weight=fc2_weight)


NORM_EPS = 1e-05
MASKED = -1e+30

def positions_of(segment):
    length = segment.shape[0]
    row_index = jnp.arange(length, dtype=jnp.int32)
    previous = jnp.concatenate([segment[:1], segment[:-1]])
    starts = jnp.where((row_index == 0) | (segment != previous), row_index, 0).astype(jnp.int32)
    return (row_index - lax.cummax(starts, axis=0)).astype(jnp.float32)

def rotary_tables(segment):
    half_rot = ROT // 2
    frequency = 10000.0 ** (-2.0 * jnp.arange(half_rot, dtype=jnp.float32) / ROT)
    phase_angle = positions_of(segment)[:, None] * frequency[None, :]
    return (jnp.cos(phase_angle)[:, None, :], jnp.sin(phase_angle)[:, None, :])

def rotate_pairs(heads_in, cos_part, sin_part):
    half_rot = ROT // 2
    lower_half = heads_in[..., :half_rot]
    upper_half = heads_in[..., half_rot:ROT]
    return jnp.concatenate([lower_half * cos_part - upper_half * sin_part, upper_half * cos_part + lower_half * sin_part, heads_in[..., ROT:]], axis=-1)

def inner_product(left, right):
    return lax.dot_general(left, right, (((0,), (0,)), ((), ())), preferred_element_type=jnp.float32)

def transposed_product(left, right):
    return lax.dot_general(left, right, (((1,), (1,)), ((), ())), preferred_element_type=jnp.float32)

def score_block(queries, key_rows, segment):
    length = segment.shape[0]
    row_index = jnp.arange(length, dtype=jnp.int32)
    allowed = (segment[:, None] == segment[None, :]) & (row_index[None, :] <= row_index[:, None])
    scores = jnp.einsum('qhd,khd->hqk', queries.astype(jnp.float32), key_rows.astype(jnp.float32)) * HEAD_DIM ** (-0.5)
    return jnp.where(allowed[None, :, :], scores, MASKED)

def gelu_grad(pre_act, grad_act):
    _, pull_back = jax.vjp(lambda value_in: jax.nn.gelu(value_in, approximate=True), pre_act)
    return pull_back(grad_act)[0]

def layer_forward(hidden, segment, weights):
    norm_gain, norm_shift, proj_qkv, bias_qv, proj_dense, bias_out, fc_one, bias_fc, fc_two = weights
    row_count = hidden.shape[0]
    head_count = D // HEAD_DIM
    residual = hidden.astype(jnp.float32)
    centred = residual - lax.optimization_barrier(jnp.mean(residual, axis=-1, keepdims=True))
    inv_std = lax.rsqrt(lax.optimization_barrier(jnp.mean(centred * centred, axis=-1, keepdims=True)) + NORM_EPS)
    standard = centred * inv_std
    normed = (standard * norm_gain + norm_shift).astype(jnp.bfloat16)
    cos_part, sin_part = rotary_tables(segment)
    query_f = jnp.dot(normed, proj_qkv[0], preferred_element_type=jnp.float32) + bias_qv[0]
    key_f = jnp.dot(normed, proj_qkv[1], preferred_element_type=jnp.float32)
    values = (jnp.dot(normed, proj_qkv[2], preferred_element_type=jnp.float32) + bias_qv[1]).astype(jnp.bfloat16).reshape(row_count, head_count, HEAD_DIM)
    queries = rotate_pairs(query_f.reshape(row_count, head_count, HEAD_DIM), cos_part, sin_part).astype(jnp.bfloat16)
    key_rows = rotate_pairs(key_f.reshape(row_count, head_count, HEAD_DIM), cos_part, sin_part).astype(jnp.bfloat16)
    scores = score_block(queries, key_rows, segment)
    row_max = lax.optimization_barrier(jnp.max(scores, axis=-1, keepdims=True))
    log_total = row_max + jnp.log(lax.optimization_barrier(jnp.sum(jnp.exp(scores - row_max), axis=-1, keepdims=True)))
    attn_prob = jnp.exp(scores - log_total).astype(jnp.bfloat16)
    attended = jnp.einsum('hqk,khd->qhd', attn_prob.astype(jnp.float32), values.astype(jnp.float32)).astype(jnp.bfloat16).reshape(row_count, D)
    pre_act = jnp.dot(normed, fc_one, preferred_element_type=jnp.float32) + bias_fc
    activation = jax.nn.gelu(pre_act, approximate=True).astype(jnp.bfloat16)
    branch = jnp.dot(attended, proj_dense, preferred_element_type=jnp.float32) + jnp.dot(activation, fc_two, preferred_element_type=jnp.float32)
    output = (residual + branch + bias_out).astype(jnp.bfloat16)
    return (output, (standard, inv_std, normed, queries, key_rows, values, log_total, attended, pre_act, activation))

def layer_backward(upstream, segment, stored, weights):
    norm_gain, norm_shift, proj_qkv, bias_qv, proj_dense, bias_out, fc_one, bias_fc, fc_two = weights
    standard, inv_std, normed, queries, key_rows, values, log_total, attended, pre_act, activation = stored
    row_count = upstream.shape[0]
    head_count = D // HEAD_DIM
    up_float = upstream.astype(jnp.float32)
    grad_dense = inner_product(attended, upstream)
    grad_fc_two = inner_product(activation, upstream)
    grad_out = lax.optimization_barrier(jnp.sum(up_float, axis=0))
    grad_pre = gelu_grad(pre_act, transposed_product(upstream, fc_two))
    grad_fc_bias = lax.optimization_barrier(jnp.sum(grad_pre, axis=0))
    grad_pre_b = grad_pre.astype(jnp.bfloat16)
    grad_fc_one = inner_product(normed, grad_pre_b)
    grad_att = transposed_product(upstream, proj_dense).astype(jnp.bfloat16).reshape(row_count, head_count, HEAD_DIM)
    cos_part, sin_part = rotary_tables(segment)
    scores = score_block(queries, key_rows, segment)
    prob_f = jnp.exp(scores - log_total)
    prob_b = prob_f.astype(jnp.bfloat16)
    grad_prob = jnp.einsum('qhd,khd->hqk', grad_att.astype(jnp.float32), values.astype(jnp.float32))
    row_dot = lax.optimization_barrier(jnp.sum(prob_f * grad_prob, axis=-1, keepdims=True))
    grad_score = (prob_f * (grad_prob - row_dot)).astype(jnp.bfloat16)
    score_scale = HEAD_DIM ** (-0.5)
    grad_query = rotate_pairs(jnp.einsum('hqk,khd->qhd', grad_score.astype(jnp.float32), key_rows.astype(jnp.float32)) * score_scale, cos_part, -sin_part).reshape(row_count, D)
    grad_key = rotate_pairs(jnp.einsum('hqk,qhd->khd', grad_score.astype(jnp.float32), queries.astype(jnp.float32)) * score_scale, cos_part, -sin_part).reshape(row_count, D)
    grad_value = jnp.einsum('hqk,qhd->khd', prob_b.astype(jnp.float32), grad_att.astype(jnp.float32)).reshape(row_count, D)
    grad_qv = jnp.stack([lax.optimization_barrier(jnp.sum(grad_query, axis=0)), lax.optimization_barrier(jnp.sum(grad_value, axis=0))])
    rounded = [piece_grad.astype(jnp.bfloat16) for piece_grad in (grad_query, grad_key, grad_value)]
    grad_qkv = jnp.stack([inner_product(normed, piece_grad) for piece_grad in rounded])
    grad_normed = transposed_product(grad_pre_b, fc_one)
    for which in range(3):
        grad_normed = grad_normed + transposed_product(rounded[which], proj_qkv[which])
    scaled = grad_normed * norm_gain
    grad_gain = lax.optimization_barrier(jnp.sum(grad_normed * standard, axis=0))
    grad_shift = lax.optimization_barrier(jnp.sum(grad_normed, axis=0))
    grad_in = inv_std * (scaled - lax.optimization_barrier(jnp.mean(scaled, axis=-1, keepdims=True)) - standard * lax.optimization_barrier(jnp.mean(scaled * standard, axis=-1, keepdims=True)))
    passed = (up_float + grad_in).astype(jnp.bfloat16)
    return (passed, (grad_gain, grad_shift, grad_qkv, grad_qv, grad_dense, grad_out, grad_fc_one, grad_fc_bias, grad_fc_two))

def reference(block_input, cotangent, segments, ln_gain, ln_bias, qkv_weight, qv_bias, dense_weight, out_bias, fc1_weight, fc1_bias, fc2_weight):
    block_count = M * N_DP
    inputs_blocked = block_input.reshape(block_count, MB, D)
    cot_blocked = cotangent.reshape(block_count, MB, D)
    seg_blocked = segments.reshape(block_count, MB)
    every = (ln_gain, ln_bias, qkv_weight, qv_bias, dense_weight, out_bias, fc1_weight, fc1_bias, fc2_weight)
    layer_zero = tuple((array[0] for array in every))
    layer_one = tuple((array[1] for array in every))
    zeros_init = tuple((jnp.zeros(array.shape, jnp.float32) for array in every))

    def block_step(running, block_item):
        hidden, cot_rows, segment = block_item
        first_out, stored_zero = layer_forward(hidden, segment, layer_zero)
        second_out, stored_one = layer_forward(first_out, segment, layer_one)
        upstream = cot_rows * (segment >= 0)[:, None].astype(jnp.bfloat16)
        grad_mid, grads_one = layer_backward(upstream, segment, stored_one, layer_one)
        grad_first, grads_zero = layer_backward(grad_mid, segment, stored_zero, layer_zero)
        running = tuple((total + jnp.stack([term_zero, term_one]) for total, term_zero, term_one in zip(running, grads_zero, grads_one)))
        return (running, (first_out, second_out, grad_first, grad_mid))
    gradients, (first_all, second_all, grad_first_all, grad_mid_all) = lax.scan(block_step, zeros_init, (inputs_blocked, cot_blocked, seg_blocked))
    layer_out = jnp.stack([first_all.reshape(M, TOKENS, D), second_all.reshape(M, TOKENS, D)])
    in_grad = jnp.stack([grad_first_all.reshape(M, TOKENS, D), grad_mid_all.reshape(M, TOKENS, D)])
    return (layer_out, in_grad) + gradients
```

```python
import functools

import jax
import jax.numpy as jnp
from jax import lax
from jax.experimental import pallas as pl
from jax.experimental.pallas import tpu as pltpu
from jax.sharding import PartitionSpec as P

HEAD_DIM = 64
ROT = 32

NORM_EPS = 1e-05
MASKED = -1e30
MESH = pl.DeviceIdType.MESH


def rotary_tables(segment):
    length = segment.shape[-1]
    row_index = jnp.arange(length, dtype=jnp.int32)[None, :]
    previous = jnp.concatenate([segment[:, :1], segment[:, :-1]], axis=1)
    starts = jnp.where((row_index == 0) | (segment != previous), row_index, 0)
    position = (row_index - lax.cummax(starts, axis=1)).astype(jnp.float32)
    half_rot = ROT // 2
    frequency = 10000.0 ** (-2.0 * jnp.arange(half_rot, dtype=jnp.float32) / ROT)
    phase_angle = position[..., None] * frequency
    return (jnp.cos(phase_angle)[:, :, None, :], jnp.sin(phase_angle)[:, :, None, :])


def rotate_pairs(heads_in, cos_part, sin_part):
    half_rot = ROT // 2
    lower_half = heads_in[..., :half_rot]
    upper_half = heads_in[..., half_rot:ROT]
    return jnp.concatenate(
        [
            lower_half * cos_part - upper_half * sin_part,
            upper_half * cos_part + lower_half * sin_part,
            heads_in[..., ROT:],
        ],
        axis=-1,
    )


def mm(left, right, dims=((1,), (0,))):
    return lax.dot_general(left, right, (dims, ((), ())), preferred_element_type=jnp.float32)


def score_blocks(queries, key_rows, segment):
    length = segment.shape[-1]
    row_index = jnp.arange(length, dtype=jnp.int32)
    allowed = (segment[:, :, None] == segment[:, None, :]) & (
        row_index[None, :] <= row_index[:, None]
    )
    scores = jnp.einsum(
        "bqhd,bkhd->bhqk", queries, key_rows, preferred_element_type=jnp.float32
    ) * HEAD_DIM ** (-0.5)
    return jnp.where(allowed[:, None, :, :], scores, MASKED)


def gelu_grad(pre_act, grad_act):
    _, pull_back = jax.vjp(lambda value_in: jax.nn.gelu(value_in, approximate=True), pre_act)
    return pull_back(grad_act)[0]


def normalize(hidden, norm_gain, norm_shift):
    residual = hidden.astype(jnp.float32)
    centred = residual - jnp.mean(residual, axis=-1, keepdims=True)
    inv_std = lax.rsqrt(jnp.mean(centred * centred, axis=-1, keepdims=True) + NORM_EPS)
    return (centred * inv_std * norm_gain + norm_shift).astype(jnp.bfloat16)


def attention_forward(normed, segment, tables, proj_qkv, bias_qv):
    blocks, rows = segment.shape
    heads = proj_qkv.shape[-1] // HEAD_DIM
    shape = (blocks, rows, heads, HEAD_DIM)
    cos_part, sin_part = tables
    query_f = (mm(normed, proj_qkv[0]) + bias_qv[0]).reshape(shape)
    key_f = mm(normed, proj_qkv[1]).reshape(shape)
    values = (mm(normed, proj_qkv[2]) + bias_qv[1]).astype(jnp.bfloat16).reshape(shape)
    queries = rotate_pairs(query_f, cos_part, sin_part).astype(jnp.bfloat16)
    key_rows = rotate_pairs(key_f, cos_part, sin_part).astype(jnp.bfloat16)
    scores = score_blocks(queries, key_rows, segment)
    row_max = jnp.max(scores, axis=-1, keepdims=True)
    log_total = row_max + jnp.log(jnp.sum(jnp.exp(scores - row_max), axis=-1, keepdims=True))
    prob_f = jnp.exp(scores - log_total)
    attended = (
        jnp.einsum(
            "bhqk,bkhd->bqhd", prob_f.astype(jnp.bfloat16), values,
            preferred_element_type=jnp.float32,
        )
        .astype(jnp.bfloat16)
        .reshape(blocks * rows, heads * HEAD_DIM)
    )
    return attended, (queries, key_rows, values, log_total)


def attention_backward(upstream, segment, tables, proj_dense, kept):
    queries, key_rows, values, log_total = kept
    shape = queries.shape
    flat = (shape[0] * shape[1], shape[2] * shape[3])
    cos_part, sin_part = tables
    grad_att = mm(upstream, proj_dense, ((1,), (1,))).astype(jnp.bfloat16).reshape(shape)
    prob_f = jnp.exp(score_blocks(queries, key_rows, segment) - log_total)
    prob_b = prob_f.astype(jnp.bfloat16)
    grad_prob = jnp.einsum("bqhd,bkhd->bhqk", grad_att, values, preferred_element_type=jnp.float32)
    row_dot = jnp.sum(prob_f * grad_prob, axis=-1, keepdims=True)
    grad_score = (prob_f * (grad_prob - row_dot)).astype(jnp.bfloat16)
    scale = HEAD_DIM ** (-0.5)
    grad_query = rotate_pairs(
        jnp.einsum("bhqk,bkhd->bqhd", grad_score, key_rows, preferred_element_type=jnp.float32)
        * scale,
        cos_part,
        -sin_part,
    ).reshape(flat)
    grad_key = rotate_pairs(
        jnp.einsum("bhqk,bqhd->bkhd", grad_score, queries, preferred_element_type=jnp.float32)
        * scale,
        cos_part,
        -sin_part,
    ).reshape(flat)
    grad_value = jnp.einsum(
        "bhqk,bqhd->bkhd", prob_b, grad_att, preferred_element_type=jnp.float32
    ).reshape(flat)
    return grad_query, grad_key, grad_value


def partner(t, k):
    out, bit = t, 1
    while bit <= k:
        if k & bit:
            out = out + (1 - 2 * (lax.rem(lax.div(t, bit), 2))) * bit
        bit *= 2
    return out


def enter(n, section_target, is_waiter):
    t = lax.axis_index("tensor")
    sec = lax.axis_index("section")
    barrier = pltpu.get_barrier_semaphore()
    for k in range(1, n):
        pl.semaphore_signal(
            barrier, inc=1, device_id={"tensor": partner(t, k)}, device_id_type=MESH
        )
    if section_target is None:
        pl.semaphore_wait(barrier, n - 1)
        return

    @pl.when(sec == section_target)
    def _():
        pl.semaphore_signal(barrier, inc=1, device_id={"section": 1 - sec}, device_id_type=MESH)
        pl.semaphore_wait(barrier, n - 1)

    @pl.when(sec != section_target)
    def _():
        pl.semaphore_wait(barrier, n)


def scatter_sum(n, partial_ref, recv, send_sem, recv_sem, own_rows):
    t = lax.axis_index("tensor")
    copies = []
    for k in range(n - 1, 0, -1):
        peer = partner(t, k)
        copy = pltpu.make_async_remote_copy(
            src_ref=partial_ref.at[:, peer],
            dst_ref=recv.at[k - 1],
            send_sem=send_sem.at[k - 1],
            recv_sem=recv_sem.at[k - 1],
            device_id={"tensor": peer},
            device_id_type=MESH,
        )
        copy.start()
        copies.append((k, copy))
    total = partial_ref[:, t].astype(jnp.float32) + own_rows
    for k, copy in copies:
        copy.wait_recv()
        total = total + recv[k - 1].astype(jnp.float32)
    return total, copies


def spread(n, full_ref, send_sem, recv_sem):
    t = lax.axis_index("tensor")
    copies = []
    for k in range(n - 1, 0, -1):
        copy = pltpu.make_async_remote_copy(
            src_ref=full_ref.at[:, t],
            dst_ref=full_ref.at[:, t],
            send_sem=send_sem.at[k - 1],
            recv_sem=recv_sem.at[k - 1],
            device_id={"tensor": partner(t, k)},
            device_id_type=MESH,
        )
        copy.start()
        copies.append(copy)
    for copy in copies:
        copy.wait()


def forward_kernel(
    n, last, partial_ref, resid_ref, bias_ref, gain_ref, shift_ref, *rest
):
    if last:
        out_ref, recv, send_sem, recv_sem = rest
        enter(n, None, None)
        total, copies = scatter_sum(
            n, partial_ref, recv, send_sem, recv_sem,
            resid_ref[...].astype(jnp.float32) + bias_ref[...][None],
        )
        out_ref[...] = total.astype(jnp.bfloat16)
        for _, copy in copies:
            copy.wait_send()
        return
    (n0_ref, x_ref, out_ref, hidden_ref, full_ref, recv, send_sem, recv_sem,
     hop_send, hop_recv, ag_send, ag_recv) = rest
    sec = lax.axis_index("section")
    t = lax.axis_index("tensor")
    enter(n, 1, None)
    total, copies = scatter_sum(
        n, partial_ref, recv, send_sem, recv_sem,
        resid_ref[...].astype(jnp.float32) + bias_ref[...][None],
    )
    out_ref[...] = total.astype(jnp.bfloat16)
    hop = pltpu.make_async_remote_copy(
        src_ref=out_ref,
        dst_ref=hidden_ref,
        send_sem=hop_send,
        recv_sem=hop_recv,
        device_id={"section": 1 - sec},
        device_id_type=MESH,
    )

    @pl.when(sec == 0)
    def _():
        hop.start()
        full_ref[...] = n0_ref[...]
        hidden_ref[...] = x_ref[...]
        hop.wait_send()

    @pl.when(sec == 1)
    def _():
        hop.wait_recv()
        residual = hidden_ref[...].astype(jnp.float32)
        centred = residual - jnp.mean(residual, axis=-1, keepdims=True)
        inv_std = lax.rsqrt(jnp.mean(centred * centred, axis=-1, keepdims=True) + NORM_EPS)
        normed = centred * inv_std * gain_ref[...][None] + shift_ref[...][None]
        full_ref[:, t] = normed.astype(jnp.bfloat16)
        spread(n, full_ref, ag_send, ag_recv)

    for _, copy in copies:
        copy.wait_send()


def backward_kernel(n, last, partial_ref, up_ref, hidden_ref, gain_ref, *rest):
    t = lax.axis_index("tensor")
    sec = lax.axis_index("section")
    if last:
        out_ref, ggain_ref, gshift_ref, recv, send_sem, recv_sem = rest
        enter(n, None, None)
    else:
        (cot_ref, out_ref, ggain_ref, gshift_ref, full_ref, recv, send_sem, recv_sem,
         hop_send, hop_recv, ag_send, ag_recv) = rest
        enter(n, 0, None)
    grad_normed, copies = scatter_sum(n, partial_ref, recv, send_sem, recv_sem, 0.0)
    residual = hidden_ref[...].astype(jnp.float32)
    centred = residual - jnp.mean(residual, axis=-1, keepdims=True)
    inv_std = lax.rsqrt(jnp.mean(centred * centred, axis=-1, keepdims=True) + NORM_EPS)
    standard = centred * inv_std
    scaled = grad_normed * gain_ref[...][None]
    grad_in = inv_std * (
        scaled
        - jnp.mean(scaled, axis=-1, keepdims=True)
        - standard * jnp.mean(scaled * standard, axis=-1, keepdims=True)
    )
    out_ref[...] = (up_ref[:, t].astype(jnp.float32) + grad_in).astype(jnp.bfloat16)
    if not last:
        hop = pltpu.make_async_remote_copy(
            src_ref=out_ref,
            dst_ref=full_ref.at[:, t],
            send_sem=hop_send,
            recv_sem=hop_recv,
            device_id={"section": 1 - sec},
            device_id_type=MESH,
        )

        @pl.when(sec == 1)
        def _():
            hop.start()
            full_ref[...] = cot_ref[...]
            hop.wait_send()

        @pl.when(sec == 0)
        def _():
            hop.wait_recv()
            spread(n, full_ref, ag_send, ag_recv)

    ggain_ref[...] = jnp.sum(jnp.sum(grad_normed * standard, axis=0), axis=0, keepdims=True)
    gshift_ref[...] = jnp.sum(jnp.sum(grad_normed, axis=0), axis=0, keepdims=True)
    for _, copy in copies:
        copy.wait_send()


def relay_call(kernel, n, last, ident, args, outs, rows_shape):
    sems = [pltpu.SemaphoreType.DMA((n - 1,)), pltpu.SemaphoreType.DMA((n - 1,))]
    scratch = [pltpu.VMEM((n - 1,) + rows_shape, jnp.bfloat16)] + sems
    if not last:
        scratch += [pltpu.SemaphoreType.DMA, pltpu.SemaphoreType.DMA] + sems
    vmem = pl.BlockSpec(memory_space=pltpu.VMEM)
    return pl.pallas_call(
        functools.partial(kernel, n, last),
        out_shape=outs,
        in_specs=[vmem] * len(args),
        out_specs=[vmem] * len(outs),
        scratch_shapes=scratch,
        compiler_params=pltpu.CompilerParams(
            collective_id=ident, has_side_effects=True, vmem_limit_bytes=32 * 1024 * 1024
        ),
    )(*args)


def small_kernel(axes, x_ref, out_ref, gathered, send_sem, recv_sem):
    sizes = [lax.axis_size(a) for a in axes]
    index = [lax.axis_index(a) for a in axes]
    count = 1
    for s in sizes:
        count *= s

    def shifted(k):
        ids, parts = {}, []
        for a, s, i in zip(reversed(axes), reversed(sizes), reversed(index)):
            ids[a] = lax.rem(i + k % s, s)
            k //= s
        return ids

    mine = 0
    for s, i in zip(sizes, index):
        mine = mine * s + i
    barrier = pltpu.get_barrier_semaphore()
    for k in range(1, count):
        pl.semaphore_signal(barrier, inc=1, device_id=shifted(k), device_id_type=MESH)
    pl.semaphore_wait(barrier, count - 1)
    copies = []
    for k in range(1, count):
        copy = pltpu.make_async_remote_copy(
            src_ref=x_ref,
            dst_ref=gathered.at[mine],
            send_sem=send_sem.at[k],
            recv_sem=recv_sem.at[k],
            device_id=shifted(k),
            device_id_type=MESH,
        )
        copy.start()
        copies.append(copy)
    gathered[mine] = x_ref[...]
    for copy in copies:
        copy.wait()
    total = gathered[0]
    for i in range(1, count):
        total = total + gathered[i]
    out_ref[...] = total


def small_sum(x, axes, ident):
    count = 1
    for a in axes:
        count *= lax.axis_size(a)
    vmem = pl.BlockSpec(memory_space=pltpu.VMEM)
    return pl.pallas_call(
        functools.partial(small_kernel, axes),
        out_shape=jax.ShapeDtypeStruct(x.shape, x.dtype),
        in_specs=[vmem],
        out_specs=vmem,
        scratch_shapes=[
            pltpu.VMEM((count,) + x.shape, x.dtype),
            pltpu.SemaphoreType.DMA((count,)),
            pltpu.SemaphoreType.DMA((count,)),
        ],
        compiler_params=pltpu.CompilerParams(collective_id=ident, has_side_effects=True),
    )(x)


def per_device(
    block_input,
    cotangent,
    segments,
    ln_gain,
    ln_bias,
    qkv_weight,
    qv_bias,
    dense_weight,
    out_bias,
    fc1_weight,
    fc1_bias,
    fc2_weight,
):
    micro, rows, width = block_input.shape
    n = lax.axis_size("tensor")
    n_dp = lax.axis_size("dp")
    share = rows // n
    group = 2 if micro % 2 == 0 else 1
    count = micro // group
    is_first = lax.axis_index("section") == 0
    row_start = lax.axis_index("tensor") * share
    norm_gain, norm_shift = ln_gain, ln_bias
    proj_qkv, proj_dense, fc_one, fc_two = (
        qkv_weight[0], dense_weight[0], fc1_weight[0], fc2_weight[0]
    )
    bias_qv, bias_fc = qv_bias[0], fc1_bias[0]
    bf16, f32 = jnp.bfloat16, jnp.float32

    live = (segments >= 0)[:, :, None].astype(bf16)
    top = cotangent * live
    own_rows = lambda x: lax.dynamic_slice_in_dim(x, row_start, share, 1)
    first_normed = normalize(block_input, norm_gain, norm_shift)
    x_rows = own_rows(block_input)
    all_segments = lax.all_gather(segments, "dp", axis=1)

    def gather(x):
        return lax.all_gather(x, ("dp", "tensor"), axis=1, tiled=True)

    early = gather(jnp.where(is_first, own_rows(first_normed), own_rows(top)))

    cut = lambda x, i: x[i * group : (i + 1) * group]
    four = lambda x: x.reshape(group, n, share, width)
    flat = lambda x: x.reshape(group * rows, width)
    sds = jax.ShapeDtypeStruct
    rows_shape = (group, share, width)

    normed = four(cut(first_normed, 0))
    hidden = cut(x_rows, 0)
    stored, outputs = [], []
    for moment in range(count + 1):
        last = moment == count
        segment = jnp.where(
            is_first, cut(segments, min(moment, count - 1)), cut(segments, max(moment - 1, 0))
        )
        tables = rotary_tables(segment)
        attended, kept = attention_forward(flat(normed), segment, tables, proj_qkv, bias_qv)
        pre_act = mm(flat(normed), fc_one) + bias_fc
        activation = jax.nn.gelu(pre_act, approximate=True).astype(bf16)
        partial = (mm(attended, proj_dense) + mm(activation, fc_two)).astype(bf16)
        stored.append((segment, tables, hidden, normed, kept, pre_act))
        args = [four(partial), hidden, out_bias, norm_gain, norm_shift]
        if last:
            (out,) = relay_call(
                forward_kernel, n, True, 1, args, [sds(rows_shape, bf16)], rows_shape
            )
        else:
            ahead = min(moment + 1, count - 1)
            args += [four(cut(first_normed, ahead)), cut(x_rows, ahead)]
            out, hidden, normed = relay_call(
                forward_kernel, n, False, 0, args,
                [sds(rows_shape, bf16), sds(rows_shape, bf16),
                 sds((group, n, share, width), bf16)],
                rows_shape,
            )
        outputs.append(out)

    up = jnp.where(is_first, jnp.zeros((), bf16), four(cut(top, count - 1)))
    in_grads, late = [], []
    gain_sum = jnp.zeros((1, width), f32)
    shift_sum = jnp.zeros((1, width), f32)
    for moment in range(count + 1):
        last = moment == count
        segment, tables, hidden, normed, kept, pre_act = stored[count - moment]
        up_flat = flat(up)
        grad_pre = gelu_grad(pre_act, mm(up_flat, fc_two, ((1,), (1,)))).astype(bf16)
        pieces = attention_backward(up_flat, segment, tables, proj_dense, kept)
        grad_normed = mm(grad_pre, fc_one, ((1,), (1,)))
        for which in range(3):
            grad_normed = grad_normed + mm(
                pieces[which].astype(bf16), proj_qkv[which], ((1,), (1,))
            )
        args = [four(grad_normed.astype(bf16)), up, hidden, norm_gain]
        outs = [sds(rows_shape, bf16), sds((1, width), f32), sds((1, width), f32)]
        if last:
            passed, g_gain, g_shift = relay_call(
                backward_kernel, n, True, 3, args, outs, rows_shape
            )
        else:
            args.append(
                four(cut(top, count - 2 - moment))
                if moment < count - 1
                else jnp.zeros((group, n, share, width), bf16)
            )
            passed, g_gain, g_shift, up = relay_call(
                backward_kernel, n, False, 2, args,
                outs + [sds((group, n, share, width), bf16)], rows_shape,
            )
            up_rows = lax.dynamic_index_in_dim(up, lax.axis_index("tensor"), 1, keepdims=False)
            normed_rows = lax.dynamic_index_in_dim(
                normed, lax.axis_index("tensor"), 1, keepdims=False
            )
            late.append(gather(jnp.where(is_first, up_rows, normed_rows)))
        in_grads.append(passed)
        gain_sum = gain_sum + g_gain
        shift_sum = shift_sum + g_shift
    late = late[::-1]

    column = lax.axis_index("dp") * (width // n_dp)
    slice_of = lambda x: lax.dynamic_slice_in_dim(x, column, width // n_dp, 1)
    total = None
    for index in range(count):
        now, then = cut(early, index), late[index]
        blocks = group * n_dp
        normed_all = jnp.where(is_first, now, then).reshape(blocks * rows, width)
        up_all = jnp.where(is_first, then, now).reshape(blocks * rows, width)
        segment = cut(all_segments, index).reshape(blocks, rows)
        tables = rotary_tables(segment)
        attended, kept = attention_forward(normed_all, segment, tables, proj_qkv, bias_qv)
        pieces = attention_backward(up_all, segment, tables, proj_dense, kept)
        pre_act = mm(normed_all, fc_one) + bias_fc
        activation = jax.nn.gelu(pre_act, approximate=True).astype(bf16)
        grad_pre = gelu_grad(pre_act, mm(up_all, fc_two, ((1,), (1,))))
        normed_part, up_part = slice_of(normed_all), slice_of(up_all)
        inner = ((0,), (0,))
        terms = [mm(normed_part, p.astype(bf16), inner) for p in pieces] + [
            mm(attended, up_part, inner),
            mm(normed_part, grad_pre.astype(bf16), inner),
            mm(activation, up_part, inner),
            jnp.sum(pieces[0], axis=0),
            jnp.sum(pieces[2], axis=0),
            jnp.sum(up_all.astype(f32), axis=0),
            jnp.sum(grad_pre, axis=0),
        ]
        total = terms if total is None else [a + b for a, b in zip(total, terms)]
    g_q, g_k, g_v, grad_dense, grad_fc_one, grad_fc_two, s_q, s_v, grad_out, grad_fc_bias = total
    norms = small_sum(jnp.concatenate([gain_sum, shift_sum], axis=0), ("dp", "tensor"), 4)

    layer_out = jnp.concatenate(
        [jnp.where(is_first, outputs[i], outputs[i + 1]) for i in range(count)], axis=0
    )
    in_grad = jnp.concatenate(
        [jnp.where(is_first, in_grads[count - i], in_grads[count - 1 - i]) for i in range(count)],
        axis=0,
    )
    return (
        layer_out[None],
        in_grad[None],
        norms[:1],
        norms[1:],
        jnp.stack([g_q, g_k, g_v])[None],
        jnp.stack([s_q, s_v])[None],
        grad_dense[None],
        grad_out[None],
        grad_fc_one[None],
        grad_fc_bias[None],
        grad_fc_two[None],
    )


def solution(mesh):
    return jax.shard_map(
        per_device,
        mesh=mesh,
        in_specs=(
            P(None, "dp", None),
            P(None, "dp", None),
            P(None, "dp"),
            P("section", None),
            P("section", None),
            P("section", None, None, "tensor"),
            P("section", None, "tensor"),
            P("section", "tensor", None),
            P("section", None),
            P("section", None, "tensor"),
            P("section", "tensor"),
            P("section", "tensor", None),
        ),
        out_specs=(
            P("section", None, ("dp", "tensor"), None),
            P("section", None, ("dp", "tensor"), None),
            P("section", None),
            P("section", None),
            P("section", None, "dp", "tensor"),
            P("section", None, "tensor"),
            P("section", "tensor", "dp"),
            P("section", None),
            P("section", "dp", "tensor"),
            P("section", "tensor"),
            P("section", "tensor", "dp"),
        ),
        check_vma=False,
    )
```

```python
import functools

import jax
import jax.numpy as jnp
from jax import lax
from jax.experimental import pallas as pl
from jax.experimental.pallas import tpu as pltpu
from jax.sharding import PartitionSpec as P

HEAD_DIM = 64
ROT = 32

NORM_EPS = 1e-05
MASKED = -1e30
MESH = pl.DeviceIdType.MESH


def rotary_tables(segment):
    blocks, length = segment.shape
    row_index = jnp.arange(length, dtype=jnp.int32)[None, :]
    previous = jnp.concatenate([segment[:, :1], segment[:, :-1]], axis=1)
    starts = jnp.where((row_index == 0) | (segment != previous), row_index, 0)
    position = (row_index - lax.cummax(starts, axis=1)).astype(jnp.float32)
    half_rot = ROT // 2
    frequency = 10000.0 ** (-2.0 * jnp.arange(half_rot, dtype=jnp.float32) / ROT)
    phase_angle = position[..., None] * frequency
    cos_part, sin_part = jnp.cos(phase_angle), jnp.sin(phase_angle)
    none = jnp.zeros((blocks, length, half_rot), jnp.float32)
    rest = jnp.ones((blocks, length, HEAD_DIM - ROT), jnp.float32)
    straight = jnp.concatenate([cos_part, cos_part, rest], axis=-1)
    from_upper = jnp.concatenate([-sin_part, none, 0.0 * rest], axis=-1)
    from_lower = jnp.concatenate([none, sin_part, 0.0 * rest], axis=-1)
    tables = jnp.stack([straight, from_upper, from_lower], axis=1)
    return jnp.concatenate([tables, tables], axis=-1)


def allowed_of(segment):
    length = segment.shape[-1]
    row_index = jnp.arange(length, dtype=jnp.int32)
    allowed = (segment[:, :, None] == segment[:, None, :]) & (
        row_index[None, :] <= row_index[:, None]
    )
    return allowed.astype(jnp.float32)


def mm(left, right, dims=((1,), (0,))):
    return lax.dot_general(left, right, (dims, ((), ())), preferred_element_type=jnp.float32)


def rotated(x, table, sign):
    half, lanes = ROT // 2, x.shape[-1]
    return (
        x * table[0]
        + pltpu.roll(x, lanes - half, 1) * (sign * table[1])
        + pltpu.roll(x, half, 1) * (sign * table[2])
    )


def softmax_of(query, key, allowed):
    scores = mm(query, key, ((1,), (1,))) * HEAD_DIM ** (-0.5)
    scores = jnp.where(allowed, scores, MASKED)
    row_max = jnp.max(scores, axis=-1, keepdims=True)
    log_total = row_max + jnp.log(jnp.sum(jnp.exp(scores - row_max), axis=-1, keepdims=True))
    return jnp.exp(scores - log_total)


def lane_masks(lanes):
    lane = lax.broadcasted_iota(jnp.int32, (1, lanes), 1)
    return [
        jnp.where(lane // HEAD_DIM == h, 1.0, 0.0).astype(jnp.bfloat16)
        for h in range(lanes // HEAD_DIM)
    ]


def attention_forward_kernel(qf_ref, kf_ref, vf_ref, table_ref, allowed_ref, q_ref, k_ref, v_ref, out_ref):
    bf16 = jnp.bfloat16
    table = table_ref[0]
    lanes = table.shape[-1]
    allowed = allowed_ref[0] > 0.5
    masks = lane_masks(lanes)
    v_ref[...] = vf_ref[...].astype(bf16)
    for pair in range(qf_ref.shape[-1] // lanes):
        at = slice(pair * lanes, (pair + 1) * lanes)
        query = rotated(qf_ref[:, at], table, 1.0).astype(bf16)
        key = rotated(kf_ref[:, at], table, 1.0).astype(bf16)
        q_ref[:, at] = query
        k_ref[:, at] = key
        value = v_ref[:, at]
        total = 0.0
        for mask in masks:
            prob = softmax_of(query * mask, key, allowed).astype(bf16)
            total = total + mm(prob, value * mask)
        out_ref[:, at] = total.astype(bf16)


def attention_backward_kernel(again, q_ref, k_ref, v_ref, ga_ref, table_ref, allowed_ref, *outs):
    bf16 = jnp.bfloat16
    table = table_ref[0]
    lanes = table.shape[-1]
    allowed = allowed_ref[0] > 0.5
    masks = lane_masks(lanes)
    scale = HEAD_DIM ** (-0.5)
    if again:
        gq_ref, gk_ref, gv_ref, out_ref, sq_ref, sv_ref = outs

        @pl.when(pl.program_id(0) == 0)
        def _():
            sq_ref[...] = jnp.zeros_like(sq_ref)
            sv_ref[...] = jnp.zeros_like(sv_ref)
    else:
        gq_ref, gk_ref, gv_ref = outs
    for pair in range(q_ref.shape[-1] // lanes):
        at = slice(pair * lanes, (pair + 1) * lanes)
        if again:
            query = rotated(q_ref[:, at], table, 1.0).astype(bf16)
            key = rotated(k_ref[:, at], table, 1.0).astype(bf16)
            value = v_ref[:, at].astype(bf16)
        else:
            query, key, value = q_ref[:, at], k_ref[:, at], v_ref[:, at]
        grad = ga_ref[:, at]
        total = g_query = g_key = g_value = 0.0
        for mask in masks:
            prob_f = softmax_of(query * mask, key, allowed)
            prob_b = prob_f.astype(bf16)
            grad_m = grad * mask
            grad_prob = mm(grad_m, value, ((1,), (1,)))
            row_dot = jnp.sum(prob_f * grad_prob, axis=-1, keepdims=True)
            grad_score = (prob_f * (grad_prob - row_dot)).astype(bf16)
            if again:
                total = total + mm(prob_b, value * mask)
            g_query = g_query + mm(grad_score, key * mask)
            g_key = g_key + mm(grad_score, query * mask, ((0,), (0,)))
            g_value = g_value + mm(prob_b, grad_m, ((0,), (0,)))
        g_query = rotated(g_query * scale, table, -1.0)
        g_key = rotated(g_key * scale, table, -1.0)
        gq_ref[:, at] = g_query.astype(bf16)
        gk_ref[:, at] = g_key.astype(bf16)
        gv_ref[:, at] = g_value.astype(bf16)
        if again:
            out_ref[:, at] = total.astype(bf16)
            sq_ref[:, at] += jnp.sum(g_query, axis=0, keepdims=True)
            sv_ref[:, at] += jnp.sum(g_value, axis=0, keepdims=True)


def attention_call(kernel, arrays, tables, allowed, outs, sums):
    blocks, _, rows, lanes = tables.shape
    features = arrays[0].shape[-1]
    block = pl.BlockSpec((rows, features), lambda i: (i, 0))
    one = pl.BlockSpec((1, features), lambda i: (0, 0))
    flat = (blocks * rows, features)
    return pl.pallas_call(
        kernel,
        grid=(blocks,),
        in_specs=[block] * len(arrays)
        + [
            pl.BlockSpec((1, 3, rows, lanes), lambda i: (i, 0, 0, 0)),
            pl.BlockSpec((1, rows, rows), lambda i: (i, 0, 0)),
        ],
        out_specs=[block] * outs + [one] * sums,
        out_shape=[jax.ShapeDtypeStruct(flat, jnp.bfloat16)] * outs
        + [jax.ShapeDtypeStruct((1, features), jnp.float32)] * sums,
        cost_estimate=pl.CostEstimate(
            flops=20 * blocks * rows * rows * features,
            bytes_accessed=blocks * rows * features * 16,
            transcendentals=0,
        ),
    )(*arrays, tables, allowed)


def projections(normed, proj_qkv, bias_qv):
    return [
        mm(normed, proj_qkv[0]) + bias_qv[0],
        mm(normed, proj_qkv[1]),
        mm(normed, proj_qkv[2]) + bias_qv[1],
    ]


def settled(x):
    return lax.optimization_barrier(x)


def gelu_grad(pre_act, grad_act):
    _, pull_back = jax.vjp(lambda value_in: jax.nn.gelu(value_in, approximate=True), pre_act)
    return pull_back(grad_act)[0]


def normalize(hidden, norm_gain, norm_shift):
    residual = hidden.astype(jnp.float32)
    centred = residual - jnp.mean(residual, axis=-1, keepdims=True)
    inv_std = lax.rsqrt(jnp.mean(centred * centred, axis=-1, keepdims=True) + NORM_EPS)
    return (centred * inv_std * norm_gain + norm_shift).astype(jnp.bfloat16)


def partner(t, k):
    out, bit = t, 1
    while bit <= k:
        if k & bit:
            out = out + (1 - 2 * (lax.rem(lax.div(t, bit), 2))) * bit
        bit *= 2
    return out


def enter(n, section_target, is_waiter):
    t = lax.axis_index("tensor")
    sec = lax.axis_index("section")
    barrier = pltpu.get_barrier_semaphore()
    for k in range(1, n):
        pl.semaphore_signal(
            barrier, inc=1, device_id={"tensor": partner(t, k)}, device_id_type=MESH
        )
    if section_target is None:
        pl.semaphore_wait(barrier, n - 1)
        return

    @pl.when(sec == section_target)
    def _():
        pl.semaphore_signal(barrier, inc=1, device_id={"section": 1 - sec}, device_id_type=MESH)
        pl.semaphore_wait(barrier, n - 1)

    @pl.when(sec != section_target)
    def _():
        pl.semaphore_wait(barrier, n)


def scatter_sum(n, partial_ref, recv, send_sem, recv_sem, own_rows):
    t = lax.axis_index("tensor")
    copies = []
    for k in range(n - 1, 0, -1):
        peer = partner(t, k)
        copy = pltpu.make_async_remote_copy(
            src_ref=partial_ref.at[:, peer],
            dst_ref=recv.at[k - 1],
            send_sem=send_sem.at[k - 1],
            recv_sem=recv_sem.at[k - 1],
            device_id={"tensor": peer},
            device_id_type=MESH,
        )
        copy.start()
        copies.append((k, copy))
    total = partial_ref[:, t].astype(jnp.float32) + own_rows
    for k, copy in copies:
        copy.wait_recv()
        total = total + recv[k - 1].astype(jnp.float32)
    return total, copies


def spread(n, full_ref, send_sem, recv_sem):
    t = lax.axis_index("tensor")
    copies = []
    for k in range(n - 1, 0, -1):
        copy = pltpu.make_async_remote_copy(
            src_ref=full_ref.at[:, t],
            dst_ref=full_ref.at[:, t],
            send_sem=send_sem.at[k - 1],
            recv_sem=recv_sem.at[k - 1],
            device_id={"tensor": partner(t, k)},
            device_id_type=MESH,
        )
        copy.start()
        copies.append(copy)
    for copy in copies:
        copy.wait()


def forward_kernel(
    n, last, partial_ref, resid_ref, bias_ref, gain_ref, shift_ref, *rest
):
    if last:
        out_ref, recv, send_sem, recv_sem = rest
        enter(n, None, None)
        total, copies = scatter_sum(
            n, partial_ref, recv, send_sem, recv_sem,
            resid_ref[...].astype(jnp.float32) + bias_ref[...][None],
        )
        out_ref[...] = total.astype(jnp.bfloat16)
        for _, copy in copies:
            copy.wait_send()
        return
    (n0_ref, x_ref, out_ref, hidden_ref, full_ref, recv, send_sem, recv_sem,
     hop_send, hop_recv, ag_send, ag_recv) = rest
    sec = lax.axis_index("section")
    t = lax.axis_index("tensor")
    enter(n, 1, None)
    total, copies = scatter_sum(
        n, partial_ref, recv, send_sem, recv_sem,
        resid_ref[...].astype(jnp.float32) + bias_ref[...][None],
    )
    out_ref[...] = total.astype(jnp.bfloat16)
    hop = pltpu.make_async_remote_copy(
        src_ref=out_ref,
        dst_ref=hidden_ref,
        send_sem=hop_send,
        recv_sem=hop_recv,
        device_id={"section": 1 - sec},
        device_id_type=MESH,
    )

    @pl.when(sec == 0)
    def _():
        hop.start()
        full_ref[...] = n0_ref[...]
        hidden_ref[...] = x_ref[...]
        hop.wait_send()

    @pl.when(sec == 1)
    def _():
        hop.wait_recv()
        residual = hidden_ref[...].astype(jnp.float32)
        centred = residual - jnp.mean(residual, axis=-1, keepdims=True)
        inv_std = lax.rsqrt(jnp.mean(centred * centred, axis=-1, keepdims=True) + NORM_EPS)
        normed = centred * inv_std * gain_ref[...][None] + shift_ref[...][None]
        full_ref[:, t] = normed.astype(jnp.bfloat16)
        spread(n, full_ref, ag_send, ag_recv)

    for _, copy in copies:
        copy.wait_send()


def backward_kernel(n, last, partial_ref, up_ref, hidden_ref, gain_ref, *rest):
    t = lax.axis_index("tensor")
    sec = lax.axis_index("section")
    if last:
        out_ref, ggain_ref, gshift_ref, recv, send_sem, recv_sem = rest
        enter(n, None, None)
    else:
        (cot_ref, out_ref, ggain_ref, gshift_ref, full_ref, recv, send_sem, recv_sem,
         hop_send, hop_recv, ag_send, ag_recv) = rest
        enter(n, 0, None)
    grad_normed, copies = scatter_sum(n, partial_ref, recv, send_sem, recv_sem, 0.0)
    residual = hidden_ref[...].astype(jnp.float32)
    centred = residual - jnp.mean(residual, axis=-1, keepdims=True)
    inv_std = lax.rsqrt(jnp.mean(centred * centred, axis=-1, keepdims=True) + NORM_EPS)
    standard = centred * inv_std
    scaled = grad_normed * gain_ref[...][None]
    grad_in = inv_std * (
        scaled
        - jnp.mean(scaled, axis=-1, keepdims=True)
        - standard * jnp.mean(scaled * standard, axis=-1, keepdims=True)
    )
    out_ref[...] = (up_ref[:, t].astype(jnp.float32) + grad_in).astype(jnp.bfloat16)
    if not last:
        hop = pltpu.make_async_remote_copy(
            src_ref=out_ref,
            dst_ref=full_ref.at[:, t],
            send_sem=hop_send,
            recv_sem=hop_recv,
            device_id={"section": 1 - sec},
            device_id_type=MESH,
        )

        @pl.when(sec == 1)
        def _():
            hop.start()
            full_ref[...] = cot_ref[...]
            hop.wait_send()

        @pl.when(sec == 0)
        def _():
            hop.wait_recv()
            spread(n, full_ref, ag_send, ag_recv)

    ggain_ref[...] = jnp.sum(jnp.sum(grad_normed * standard, axis=0), axis=0, keepdims=True)
    gshift_ref[...] = jnp.sum(jnp.sum(grad_normed, axis=0), axis=0, keepdims=True)
    for _, copy in copies:
        copy.wait_send()


def relay_call(kernel, n, last, ident, args, outs, rows_shape):
    sems = [pltpu.SemaphoreType.DMA((n - 1,)), pltpu.SemaphoreType.DMA((n - 1,))]
    scratch = [pltpu.VMEM((n - 1,) + rows_shape, jnp.bfloat16)] + sems
    if not last:
        scratch += [pltpu.SemaphoreType.DMA, pltpu.SemaphoreType.DMA] + sems
    vmem = pl.BlockSpec(memory_space=pltpu.VMEM)
    return pl.pallas_call(
        functools.partial(kernel, n, last),
        out_shape=outs,
        in_specs=[vmem] * len(args),
        out_specs=[vmem] * len(outs),
        scratch_shapes=scratch,
        compiler_params=pltpu.CompilerParams(
            collective_id=ident, has_side_effects=True, vmem_limit_bytes=32 * 1024 * 1024
        ),
    )(*args)


def exchange_kernel(axes, add, x_ref, out_ref, *rest):
    gathered, send_sem, recv_sem = rest if add else (out_ref,) + rest
    sizes = [lax.axis_size(a) for a in axes]
    index = [lax.axis_index(a) for a in axes]
    count = 1
    mine = 0
    for s, i in zip(sizes, index):
        count *= s
        mine = mine * s + i

    def shifted(k):
        ids = {}
        for a, s, i in zip(reversed(axes), reversed(sizes), reversed(index)):
            ids[a] = lax.rem(i + k % s, s)
            k //= s
        return ids

    barrier = pltpu.get_barrier_semaphore()
    for k in range(1, count):
        pl.semaphore_signal(barrier, inc=1, device_id=shifted(k), device_id_type=MESH)
    pl.semaphore_wait(barrier, count - 1)
    copies = []
    for k in range(1, count):
        copy = pltpu.make_async_remote_copy(
            src_ref=x_ref,
            dst_ref=gathered.at[mine],
            send_sem=send_sem.at[k],
            recv_sem=recv_sem.at[k],
            device_id=shifted(k),
            device_id_type=MESH,
        )
        copy.start()
        copies.append(copy)
    gathered[mine] = x_ref[...]
    for copy in copies:
        copy.wait()
    if add:
        total = gathered[0]
        for i in range(1, count):
            total = total + gathered[i]
        out_ref[...] = total


def small_exchange(x, axes, ident, add):
    count = 1
    for a in axes:
        count *= lax.axis_size(a)
    vmem = pl.BlockSpec(memory_space=pltpu.VMEM)
    stacked = (count,) + x.shape
    return pl.pallas_call(
        functools.partial(exchange_kernel, axes, add),
        out_shape=jax.ShapeDtypeStruct(x.shape if add else stacked, x.dtype),
        in_specs=[vmem],
        out_specs=vmem,
        scratch_shapes=([pltpu.VMEM(stacked, x.dtype)] if add else [])
        + [pltpu.SemaphoreType.DMA((count,)), pltpu.SemaphoreType.DMA((count,))],
        compiler_params=pltpu.CompilerParams(collective_id=ident, has_side_effects=True),
    )(x)


def per_device(
    block_input,
    cotangent,
    segments,
    ln_gain,
    ln_bias,
    qkv_weight,
    qv_bias,
    dense_weight,
    out_bias,
    fc1_weight,
    fc1_bias,
    fc2_weight,
):
    micro, rows, width = block_input.shape
    n = lax.axis_size("tensor")
    n_dp = lax.axis_size("dp")
    share = rows // n
    group = 2 if micro % 2 == 0 else 1
    count = micro // group
    is_first = lax.axis_index("section") == 0
    row_start = lax.axis_index("tensor") * share
    norm_gain, norm_shift = ln_gain, ln_bias
    proj_qkv, proj_dense, fc_one, fc_two = (
        qkv_weight[0], dense_weight[0], fc1_weight[0], fc2_weight[0]
    )
    bias_qv, bias_fc = qv_bias[0], fc1_bias[0]
    bf16, f32 = jnp.bfloat16, jnp.float32

    live = (segments >= 0)[:, :, None].astype(bf16)
    top = cotangent * live
    own_rows = lambda x: lax.dynamic_slice_in_dim(x, row_start, share, 1)
    first_normed = normalize(block_input, norm_gain, norm_shift)
    x_rows = own_rows(block_input)
    all_segments = small_exchange(segments, ("dp",), 5, False)

    def gather(x):
        return lax.all_gather(x, ("dp", "tensor"), axis=1, tiled=True)

    early = gather(jnp.where(is_first, own_rows(first_normed), own_rows(top)))

    cut = lambda x, i: x[i * group : (i + 1) * group]
    four = lambda x: x.reshape(group, n, share, width)
    flat = lambda x: x.reshape(group * rows, width)
    sds = jax.ShapeDtypeStruct
    rows_shape = (group, share, width)

    normed = four(cut(first_normed, 0))
    hidden = cut(x_rows, 0)
    stored, outputs = [], []
    for moment in range(count + 1):
        last = moment == count
        if last:
            normed, early = settled((normed, early))
        segment = jnp.where(
            is_first, cut(segments, min(moment, count - 1)), cut(segments, max(moment - 1, 0))
        )
        tables, allowed = rotary_tables(segment), allowed_of(segment)
        *kept, attended = attention_call(
            attention_forward_kernel,
            projections(flat(normed), proj_qkv, bias_qv), tables, allowed, 4, 0,
        )
        pre_act = mm(flat(normed), fc_one) + bias_fc
        activation = settled(jax.nn.gelu(pre_act, approximate=True).astype(bf16))
        partial = (mm(attended, proj_dense) + mm(activation, fc_two)).astype(bf16)
        stored.append((tables, allowed, hidden, normed, kept, pre_act))
        args = [four(partial), hidden, out_bias, norm_gain, norm_shift]
        if last:
            (out,) = relay_call(
                forward_kernel, n, True, 1, args, [sds(rows_shape, bf16)], rows_shape
            )
        else:
            ahead = min(moment + 1, count - 1)
            args += [four(cut(first_normed, ahead)), cut(x_rows, ahead)]
            out, hidden, normed = relay_call(
                forward_kernel, n, False, 0, args,
                [sds(rows_shape, bf16), sds(rows_shape, bf16),
                 sds((group, n, share, width), bf16)],
                rows_shape,
            )
        outputs.append(out)

    up = jnp.where(is_first, jnp.zeros((), bf16), four(cut(top, count - 1)))
    in_grads, late = [], []
    gain_sum = jnp.zeros((1, width), f32)
    shift_sum = jnp.zeros((1, width), f32)
    for moment in range(count + 1):
        last = moment == count
        tables, allowed, hidden, normed, kept, pre_act = stored[count - moment]
        up_flat = flat(up)
        grad_pre = settled(
            gelu_grad(pre_act, mm(up_flat, fc_two, ((1,), (1,)))).astype(bf16)
        )
        grad_att = mm(up_flat, proj_dense, ((1,), (1,))).astype(bf16)
        pieces = attention_call(
            functools.partial(attention_backward_kernel, False),
            kept + [grad_att], tables, allowed, 3, 0,
        )
        grad_normed = mm(grad_pre, fc_one, ((1,), (1,)))
        for which in range(3):
            grad_normed = grad_normed + mm(
                pieces[which], proj_qkv[which], ((1,), (1,))
            )
        args = [four(grad_normed.astype(bf16)), up, hidden, norm_gain]
        outs = [sds(rows_shape, bf16), sds((1, width), f32), sds((1, width), f32)]
        if last:
            passed, g_gain, g_shift = relay_call(
                backward_kernel, n, True, 3, args, outs, rows_shape
            )
        else:
            args.append(
                four(cut(top, count - 2 - moment))
                if moment < count - 1
                else jnp.zeros((group, n, share, width), bf16)
            )
            passed, g_gain, g_shift, up = relay_call(
                backward_kernel, n, False, 2, args,
                outs + [sds((group, n, share, width), bf16)], rows_shape,
            )
            up_rows = lax.dynamic_index_in_dim(up, lax.axis_index("tensor"), 1, keepdims=False)
            normed_rows = lax.dynamic_index_in_dim(
                normed, lax.axis_index("tensor"), 1, keepdims=False
            )
            late.append(gather(jnp.where(is_first, up_rows, normed_rows)))
        in_grads.append(passed)
        gain_sum = gain_sum + g_gain
        shift_sum = shift_sum + g_shift
    late = late[::-1]

    column = lax.axis_index("dp") * (width // n_dp)
    slice_of = lambda x: lax.dynamic_slice_in_dim(x, column, width // n_dp, 1)
    total = None
    for index in range(count):
        now, then = cut(early, index), late[index]
        blocks = group * n_dp
        normed_all = settled(jnp.where(is_first, now, then).reshape(blocks * rows, width))
        up_all = settled(jnp.where(is_first, then, now).reshape(blocks * rows, width))
        segment = all_segments[:, index * group : (index + 1) * group]
        segment = jnp.swapaxes(segment, 0, 1).reshape(blocks, rows)
        tables, allowed = rotary_tables(segment), allowed_of(segment)
        grad_att = mm(up_all, proj_dense, ((1,), (1,))).astype(bf16)
        *pieces, attended, s_q, s_v = attention_call(
            functools.partial(attention_backward_kernel, True),
            projections(normed_all, proj_qkv, bias_qv) + [grad_att], tables, allowed, 4, 2,
        )
        pre_act = mm(normed_all, fc_one) + bias_fc
        activation = settled(jax.nn.gelu(pre_act, approximate=True).astype(bf16))
        grad_pre = gelu_grad(pre_act, mm(up_all, fc_two, ((1,), (1,))))
        grad_fc_bias = jnp.sum(grad_pre, axis=0)
        grad_pre, grad_fc_bias = settled((grad_pre.astype(bf16), grad_fc_bias))
        normed_part, up_part = slice_of(normed_all), slice_of(up_all)
        inner = ((0,), (0,))
        terms = [mm(normed_part, p, inner) for p in pieces] + [
            mm(attended, up_part, inner),
            mm(normed_part, grad_pre, inner),
            mm(activation, up_part, inner),
            s_q[0],
            s_v[0],
            jnp.sum(up_all.astype(f32), axis=0),
            grad_fc_bias,
        ]
        total = terms if total is None else [a + b for a, b in zip(total, terms)]
    g_q, g_k, g_v, grad_dense, grad_fc_one, grad_fc_two, s_q, s_v, grad_out, grad_fc_bias = total
    norms = small_exchange(
        jnp.concatenate([gain_sum, shift_sum], axis=0), ("dp", "tensor"), 4, True
    )

    layer_out = jnp.concatenate(
        [jnp.where(is_first, outputs[i], outputs[i + 1]) for i in range(count)], axis=0
    )
    in_grad = jnp.concatenate(
        [jnp.where(is_first, in_grads[count - i], in_grads[count - 1 - i]) for i in range(count)],
        axis=0,
    )
    return (
        layer_out[None],
        in_grad[None],
        norms[:1],
        norms[1:],
        jnp.stack([g_q, g_k, g_v])[None],
        jnp.stack([s_q, s_v])[None],
        grad_dense[None],
        grad_out[None],
        grad_fc_one[None],
        grad_fc_bias[None],
        grad_fc_two[None],
    )


def solution(mesh):
    return jax.shard_map(
        per_device,
        mesh=mesh,
        in_specs=(
            P(None, "dp", None),
            P(None, "dp", None),
            P(None, "dp"),
            P("section", None),
            P("section", None),
            P("section", None, None, "tensor"),
            P("section", None, "tensor"),
            P("section", "tensor", None),
            P("section", None),
            P("section", None, "tensor"),
            P("section", "tensor"),
            P("section", "tensor", None),
        ),
        out_specs=(
            P("section", None, ("dp", "tensor"), None),
            P("section", None, ("dp", "tensor"), None),
            P("section", None),
            P("section", None),
            P("section", None, "dp", "tensor"),
            P("section", None, "tensor"),
            P("section", "tensor", "dp"),
            P("section", None),
            P("section", "dp", "tensor"),
            P("section", "tensor"),
            P("section", "tensor", "dp"),
        ),
        check_vma=False,
    )
```

```python
import functools

import jax
import jax.numpy as jnp
from jax import lax
from jax.experimental import pallas as pl
from jax.experimental.pallas import tpu as pltpu
from jax.sharding import PartitionSpec as P

HEAD_DIM = 64
ROT = 32

NORM_EPS = 1e-05
MASKED = -1e30
MESH = pl.DeviceIdType.MESH


def rotary_tables(segment):
    blocks, length = segment.shape
    row_index = jnp.arange(length, dtype=jnp.int32)[None, :]
    previous = jnp.concatenate([segment[:, :1], segment[:, :-1]], axis=1)
    starts = jnp.where((row_index == 0) | (segment != previous), row_index, 0)
    position = (row_index - lax.cummax(starts, axis=1)).astype(jnp.float32)
    half_rot = ROT // 2
    frequency = 10000.0 ** (-2.0 * jnp.arange(half_rot, dtype=jnp.float32) / ROT)
    phase_angle = position[..., None] * frequency
    cos_part, sin_part = jnp.cos(phase_angle), jnp.sin(phase_angle)
    none = jnp.zeros((blocks, length, half_rot), jnp.float32)
    rest = jnp.ones((blocks, length, HEAD_DIM - ROT), jnp.float32)
    straight = jnp.concatenate([cos_part, cos_part, rest], axis=-1)
    from_upper = jnp.concatenate([-sin_part, none, 0.0 * rest], axis=-1)
    from_lower = jnp.concatenate([none, sin_part, 0.0 * rest], axis=-1)
    tables = jnp.stack([straight, from_upper, from_lower], axis=1)
    return jnp.concatenate([tables, tables], axis=-1)


def allowed_of(segment):
    length = segment.shape[-1]
    row_index = jnp.arange(length, dtype=jnp.int32)
    allowed = (segment[:, :, None] == segment[:, None, :]) & (
        row_index[None, :] <= row_index[:, None]
    )
    return allowed.astype(jnp.float32)


def mm(left, right, dims=((1,), (0,))):
    return lax.dot_general(left, right, (dims, ((), ())), preferred_element_type=jnp.float32)


def rotated(x, table, sign):
    half, lanes = ROT // 2, x.shape[-1]
    return (
        x * table[0]
        + pltpu.roll(x, lanes - half, 1) * (sign * table[1])
        + pltpu.roll(x, half, 1) * (sign * table[2])
    )


def softmax_of(query, key, allowed):
    scores = mm(query, key, ((1,), (1,))) * HEAD_DIM ** (-0.5)
    scores = jnp.where(allowed, scores, MASKED)
    row_max = jnp.max(scores, axis=-1, keepdims=True)
    log_total = row_max + jnp.log(jnp.sum(jnp.exp(scores - row_max), axis=-1, keepdims=True))
    return jnp.exp(scores - log_total)


def lane_masks(lanes):
    lane = lax.broadcasted_iota(jnp.int32, (1, lanes), 1)
    return [
        jnp.where(lane // HEAD_DIM == h, 1.0, 0.0).astype(jnp.bfloat16)
        for h in range(lanes // HEAD_DIM)
    ]


def attention_forward_kernel(qf_ref, kf_ref, vf_ref, table_ref, allowed_ref, q_ref, k_ref, v_ref, out_ref):
    bf16 = jnp.bfloat16
    table = table_ref[0]
    lanes = table.shape[-1]
    allowed = allowed_ref[0] > 0.5
    masks = lane_masks(lanes)
    v_ref[...] = vf_ref[...].astype(bf16)
    for pair in range(qf_ref.shape[-1] // lanes):
        at = slice(pair * lanes, (pair + 1) * lanes)
        query = rotated(qf_ref[:, at], table, 1.0).astype(bf16)
        key = rotated(kf_ref[:, at], table, 1.0).astype(bf16)
        q_ref[:, at] = query
        k_ref[:, at] = key
        value = v_ref[:, at]
        total = 0.0
        for mask in masks:
            prob = softmax_of(query * mask, key, allowed).astype(bf16)
            total = total + mm(prob, value * mask)
        out_ref[:, at] = total.astype(bf16)


def attention_backward_kernel(again, q_ref, k_ref, v_ref, ga_ref, table_ref, allowed_ref, *outs):
    bf16 = jnp.bfloat16
    table = table_ref[0]
    lanes = table.shape[-1]
    allowed = allowed_ref[0] > 0.5
    masks = lane_masks(lanes)
    scale = HEAD_DIM ** (-0.5)
    if again:
        gq_ref, gk_ref, gv_ref, out_ref, sq_ref, sv_ref = outs

        @pl.when(pl.program_id(0) == 0)
        def _():
            sq_ref[...] = jnp.zeros_like(sq_ref)
            sv_ref[...] = jnp.zeros_like(sv_ref)
    else:
        gq_ref, gk_ref, gv_ref = outs
    for pair in range(q_ref.shape[-1] // lanes):
        at = slice(pair * lanes, (pair + 1) * lanes)
        if again:
            query = rotated(q_ref[:, at], table, 1.0).astype(bf16)
            key = rotated(k_ref[:, at], table, 1.0).astype(bf16)
            value = v_ref[:, at].astype(bf16)
        else:
            query, key, value = q_ref[:, at], k_ref[:, at], v_ref[:, at]
        grad = ga_ref[:, at]
        total = g_query = g_key = g_value = 0.0
        for mask in masks:
            prob_f = softmax_of(query * mask, key, allowed)
            prob_b = prob_f.astype(bf16)
            grad_m = grad * mask
            grad_prob = mm(grad_m, value, ((1,), (1,)))
            row_dot = jnp.sum(prob_f * grad_prob, axis=-1, keepdims=True)
            grad_score = (prob_f * (grad_prob - row_dot)).astype(bf16)
            if again:
                total = total + mm(prob_b, value * mask)
            g_query = g_query + mm(grad_score, key * mask)
            g_key = g_key + mm(grad_score, query * mask, ((0,), (0,)))
            g_value = g_value + mm(prob_b, grad_m, ((0,), (0,)))
        g_query = rotated(g_query * scale, table, -1.0)
        g_key = rotated(g_key * scale, table, -1.0)
        gq_ref[:, at] = g_query.astype(bf16)
        gk_ref[:, at] = g_key.astype(bf16)
        gv_ref[:, at] = g_value.astype(bf16)
        if again:
            out_ref[:, at] = total.astype(bf16)
            sq_ref[:, at] += jnp.sum(g_query, axis=0, keepdims=True)
            sv_ref[:, at] += jnp.sum(g_value, axis=0, keepdims=True)


def attention_call(kernel, arrays, tables, allowed, outs, sums):
    blocks, _, rows, lanes = tables.shape
    features = arrays[0].shape[-1]
    block = pl.BlockSpec((rows, features), lambda i: (i, 0))
    one = pl.BlockSpec((1, features), lambda i: (0, 0))
    flat = (blocks * rows, features)
    return pl.pallas_call(
        kernel,
        grid=(blocks,),
        in_specs=[block] * len(arrays)
        + [
            pl.BlockSpec((1, 3, rows, lanes), lambda i: (i, 0, 0, 0)),
            pl.BlockSpec((1, rows, rows), lambda i: (i, 0, 0)),
        ],
        out_specs=[block] * outs + [one] * sums,
        out_shape=[jax.ShapeDtypeStruct(flat, jnp.bfloat16)] * outs
        + [jax.ShapeDtypeStruct((1, features), jnp.float32)] * sums,
        cost_estimate=pl.CostEstimate(
            flops=20 * blocks * rows * rows * features,
            bytes_accessed=blocks * rows * features * 16,
            transcendentals=0,
        ),
    )(*arrays, tables, allowed)


def projections(normed, proj_qkv, bias_qv):
    return [
        mm(normed, proj_qkv[0]) + bias_qv[0],
        mm(normed, proj_qkv[1]),
        mm(normed, proj_qkv[2]) + bias_qv[1],
    ]


def settled(x):
    return lax.optimization_barrier(x)


def gelu_grad(pre_act, grad_act):
    _, pull_back = jax.vjp(lambda value_in: jax.nn.gelu(value_in, approximate=True), pre_act)
    return pull_back(grad_act)[0]


def normalize(hidden, norm_gain, norm_shift):
    residual = hidden.astype(jnp.float32)
    centred = residual - jnp.mean(residual, axis=-1, keepdims=True)
    inv_std = lax.rsqrt(jnp.mean(centred * centred, axis=-1, keepdims=True) + NORM_EPS)
    return (centred * inv_std * norm_gain + norm_shift).astype(jnp.bfloat16)


def partner(t, k):
    out, bit = t, 1
    while bit <= k:
        if k & bit:
            out = out + (1 - 2 * (lax.rem(lax.div(t, bit), 2))) * bit
        bit *= 2
    return out


def enter(n):
    t, sec = lax.axis_index("tensor"), lax.axis_index("section")
    barrier = pltpu.get_barrier_semaphore()
    for k in range(1, n):
        pl.semaphore_signal(
            barrier, inc=1, device_id={"tensor": partner(t, k)}, device_id_type=MESH
        )
    pl.semaphore_signal(barrier, inc=1, device_id={"section": 1 - sec}, device_id_type=MESH)
    pl.semaphore_wait(barrier, n)


def send(src, dst, sems, device):
    copy = pltpu.make_async_remote_copy(
        src_ref=src, dst_ref=dst, send_sem=sems[0], recv_sem=sems[1],
        device_id=device, device_id_type=MESH,
    )
    copy.start()
    return copy


def halves_of(width):
    sec = lax.axis_index("section")
    half = width // 2
    return (
        pl.ds(pl.multiple_of(sec * half, half), half),
        pl.ds(pl.multiple_of((1 - sec) * half, half), half),
    )


def reduced_half(n, partial_ref, scratch):
    pair, out_buf, recv, pair_sems, rs_sems = scratch
    t, sec = lax.axis_index("tensor"), lax.axis_index("section")
    mine, other = halves_of(partial_ref.shape[-1])
    enter(n)
    order = list(range(n - 1, -1, -1))
    swaps = {}
    for k in order:
        at = partner(t, k)
        swaps[k] = send(
            partial_ref.at[:, at, :, other], pair.at[k],
            [x.at[k] for x in pair_sems], {"section": 1 - sec},
        )
    sends = []
    for k in order:
        at = partner(t, k)
        swaps[k].wait_recv()
        both = partial_ref[:, at, :, mine].astype(jnp.float32) + pair[k].astype(jnp.float32)
        if k == 0:
            total = both
        else:
            out_buf[k - 1] = both.astype(jnp.bfloat16)
            sends.append(
                (k, send(out_buf.at[k - 1], recv.at[k - 1],
                         [x.at[k - 1] for x in rs_sems], {"tensor": at}))
            )
    for k, copy in sends:
        copy.wait_recv()
        total = total + recv[k - 1].astype(jnp.float32)
    return total, list(swaps.values()) + [copy for _, copy in sends]


def spread(n, full_ref, ag_sems, fw_sems):
    t, sec = lax.axis_index("tensor"), lax.axis_index("section")
    mine, _ = halves_of(full_ref.shape[-1])
    own = full_ref.at[:, t, :, mine]
    copies = [
        send(own, own, [x.at[k - 1] for x in ag_sems], {"tensor": partner(t, k)})
        for k in range(n - 1, 0, -1)
    ]
    passed = []
    for k, copy in zip(range(n - 1, 0, -1), copies):
        copy.wait_recv()
        part = full_ref.at[:, partner(t, k), :, mine]
        passed.append(send(part, part, [x.at[k - 1] for x in fw_sems], {"section": 1 - sec}))
    for copy in copies:
        copy.wait_send()
    for copy in passed:
        copy.wait()


def standard_of(rows):
    centred = rows - jnp.mean(rows, axis=-1, keepdims=True)
    inv_std = lax.rsqrt(jnp.mean(centred * centred, axis=-1, keepdims=True) + NORM_EPS)
    return centred * inv_std, inv_std


def forward_kernel(n, last, partial_ref, resid_ref, bias_ref, *rest):
    if last:
        out_ref, *scratch = rest
    else:
        gain_ref, shift_ref, out_ref, full_ref, *scratch = rest
    t, sec = lax.axis_index("tensor"), lax.axis_index("section")
    mine, _ = halves_of(partial_ref.shape[-1])
    total, copies = reduced_half(n, partial_ref, unpack(scratch))
    total = total + resid_ref[:, :, mine].astype(jnp.float32) + bias_ref[:, mine][None]
    out_ref[:, :, mine] = total.astype(jnp.bfloat16)
    part = out_ref.at[:, :, mine]
    hop = send(part, part, scratch[7:9], {"section": 1 - sec})
    hop.wait()
    if not last:
        standard, _ = standard_of(out_ref[...].astype(jnp.float32))
        full_ref[:, t] = (standard * gain_ref[...][None] + shift_ref[...][None]).astype(
            jnp.bfloat16
        )
        spread(n, full_ref, scratch[9:11], scratch[11:13])
    for copy in copies:
        copy.wait_send()


def unpack(scratch):
    pair, out_buf, recv, pair_s, pair_r, rs_s, rs_r = scratch[:7]
    return pair, out_buf, recv, (pair_s, pair_r), (rs_s, rs_r)


def backward_kernel(n, last, partial_ref, up_ref, hidden_ref, gain_ref, *rest):
    if last:
        out_ref, ggain_ref, gshift_ref, *scratch = rest
    else:
        out_ref, ggain_ref, gshift_ref, full_ref, *scratch = rest
    *scratch, whole = scratch
    t, sec = lax.axis_index("tensor"), lax.axis_index("section")
    mine, _ = halves_of(partial_ref.shape[-1])
    total, copies = reduced_half(n, partial_ref, unpack(scratch))
    whole[:, :, mine] = total
    part = whole.at[:, :, mine]
    hop = send(part, part, scratch[7:9], {"section": 1 - sec})
    standard, inv_std = standard_of(hidden_ref[...].astype(jnp.float32))
    hop.wait()
    grad_normed = whole[...]
    scaled = grad_normed * gain_ref[...][None]
    grad_in = inv_std * (
        scaled
        - jnp.mean(scaled, axis=-1, keepdims=True)
        - standard * jnp.mean(scaled * standard, axis=-1, keepdims=True)
    )
    out_ref[...] = (up_ref[:, t].astype(jnp.float32) + grad_in).astype(jnp.bfloat16)
    if not last:
        full_ref[:, t] = out_ref[...]
        spread(n, full_ref, scratch[9:11], scratch[11:13])
    ggain_ref[...] = jnp.sum(jnp.sum(grad_normed * standard, axis=0), axis=0, keepdims=True)
    gshift_ref[...] = jnp.sum(jnp.sum(grad_normed, axis=0), axis=0, keepdims=True)
    for copy in copies:
        copy.wait_send()


def sum_call(kernel, n, last, ident, args, outs, rows_shape):
    dma = pltpu.SemaphoreType.DMA
    half = rows_shape[:-1] + (rows_shape[-1] // 2,)
    scratch = [
        pltpu.VMEM((n,) + half, jnp.bfloat16),
        pltpu.VMEM((n - 1,) + half, jnp.bfloat16),
        pltpu.VMEM((n - 1,) + half, jnp.bfloat16),
        dma((n,)), dma((n,)), dma((n - 1,)), dma((n - 1,)), dma, dma,
    ]
    if not last:
        scratch += [dma((n - 1,))] * 4
    if kernel is backward_kernel:
        scratch.append(pltpu.VMEM(rows_shape, jnp.float32))
    vmem = pl.BlockSpec(memory_space=pltpu.VMEM)
    return pl.pallas_call(
        functools.partial(kernel, n, last),
        out_shape=outs,
        in_specs=[vmem] * len(args),
        out_specs=[vmem] * len(outs),
        scratch_shapes=scratch,
        compiler_params=pltpu.CompilerParams(
            collective_id=ident, has_side_effects=True, vmem_limit_bytes=32 * 1024 * 1024
        ),
    )(*args)


def exchange_kernel(axes, add, x_ref, out_ref, *rest):
    gathered, send_sem, recv_sem = rest if add else (out_ref,) + rest
    sizes = [lax.axis_size(a) for a in axes]
    index = [lax.axis_index(a) for a in axes]
    count = 1
    mine = 0
    for s, i in zip(sizes, index):
        count *= s
        mine = mine * s + i

    def shifted(k):
        ids = {}
        for a, s, i in zip(reversed(axes), reversed(sizes), reversed(index)):
            ids[a] = lax.rem(i + k % s, s)
            k //= s
        return ids

    barrier = pltpu.get_barrier_semaphore()
    for k in range(1, count):
        pl.semaphore_signal(barrier, inc=1, device_id=shifted(k), device_id_type=MESH)
    pl.semaphore_wait(barrier, count - 1)
    copies = []
    for k in range(1, count):
        copy = pltpu.make_async_remote_copy(
            src_ref=x_ref,
            dst_ref=gathered.at[mine],
            send_sem=send_sem.at[k],
            recv_sem=recv_sem.at[k],
            device_id=shifted(k),
            device_id_type=MESH,
        )
        copy.start()
        copies.append(copy)
    gathered[mine] = x_ref[...]
    for copy in copies:
        copy.wait()
    if add:
        total = gathered[0]
        for i in range(1, count):
            total = total + gathered[i]
        out_ref[...] = total


def small_exchange(x, axes, ident, add):
    count = 1
    for a in axes:
        count *= lax.axis_size(a)
    vmem = pl.BlockSpec(memory_space=pltpu.VMEM)
    stacked = (count,) + x.shape
    return pl.pallas_call(
        functools.partial(exchange_kernel, axes, add),
        out_shape=jax.ShapeDtypeStruct(x.shape if add else stacked, x.dtype),
        in_specs=[vmem],
        out_specs=vmem,
        scratch_shapes=([pltpu.VMEM(stacked, x.dtype)] if add else [])
        + [pltpu.SemaphoreType.DMA((count,)), pltpu.SemaphoreType.DMA((count,))],
        compiler_params=pltpu.CompilerParams(collective_id=ident, has_side_effects=True),
    )(x)


def per_device(
    block_input,
    cotangent,
    segments,
    ln_gain,
    ln_bias,
    qkv_weight,
    qv_bias,
    dense_weight,
    out_bias,
    fc1_weight,
    fc1_bias,
    fc2_weight,
):
    micro, rows, width = block_input.shape
    n = lax.axis_size("tensor")
    n_dp = lax.axis_size("dp")
    share = rows // n
    group = 2 if micro % 2 == 0 else 1
    count = micro // group
    sec = lax.axis_index("section")
    is_first = sec == 0
    row_start = lax.axis_index("tensor") * share
    proj_qkv, proj_dense, fc_one, fc_two = (
        qkv_weight[0], dense_weight[0], fc1_weight[0], fc2_weight[0]
    )
    bias_qv, bias_fc = qv_bias[0], fc1_bias[0]
    bf16, f32 = jnp.bfloat16, jnp.float32
    features, hidden_units = proj_qkv.shape[-1], fc_one.shape[-1]

    swap = lambda x: lax.ppermute(x, "section", [(0, 1), (1, 0)])

    def half(x, axis, which):
        size = x.shape[axis] // 2
        return lax.dynamic_slice_in_dim(x, which * size, size, axis)

    def both(x, axis):
        return half(x, axis, sec), swap(half(x, axis, 1 - sec))

    def of_layer(index, pair):
        return jnp.where(sec == index, pair[0], pair[1])

    small = jnp.concatenate(
        [ln_gain[0], ln_bias[0], out_bias[0], bias_qv.reshape(-1), bias_fc]
    )[None]
    small_pair = (small, swap(small))
    weight_pairs = [
        both(proj_qkv, 2), both(fc_one, 1), both(proj_dense, 0), both(fc_two, 0)
    ]

    def parameters(index):
        vector = of_layer(index, small_pair)[0]
        gain, shift, bias = [vector[None, i * width : (i + 1) * width] for i in range(3)]
        at = 3 * width
        b_qv = half(vector[at : at + 2 * features].reshape(2, features), 1, sec)
        b_fc = half(vector[at + 2 * features :], 0, sec)
        return gain, shift, bias, b_qv, b_fc, [of_layer(index, p) for p in weight_pairs]

    layers = [parameters(0), parameters(1)]

    live = (segments >= 0)[:, :, None].astype(bf16)
    top = cotangent * live
    own_rows = lambda x: lax.dynamic_slice_in_dim(x, row_start, share, 1)
    first_normed = normalize(block_input, layers[0][0], layers[0][1])
    x_rows = own_rows(block_input)
    all_segments = small_exchange(segments, ("dp",), 5, False)
    tables, allowed = rotary_tables(segments), allowed_of(segments)

    def gather(x):
        return lax.all_gather(x, ("dp", "tensor"), axis=1, tiled=True)

    early = gather(jnp.where(is_first, own_rows(first_normed), own_rows(top)))

    four = lambda x: x.reshape(micro, n, share, width)
    flat = lambda x: x.reshape(micro * rows, width)
    sds = jax.ShapeDtypeStruct
    rows_shape = (micro, share, width)
    rows_out, full_out = sds(rows_shape, bf16), sds((micro, n, share, width), bf16)
    line = sds((1, width), f32)

    def branch_forward(normed, layer):
        _, _, _, b_qv, b_fc, (w_qkv, w_one, w_dense, w_two) = layer
        *kept, attended = attention_call(
            attention_forward_kernel, projections(normed, w_qkv, b_qv), tables, allowed, 4, 0,
        )
        pre_act = mm(normed, w_one) + b_fc
        activation = settled(jax.nn.gelu(pre_act, approximate=True).astype(bf16))
        partial = (mm(attended, w_dense) + mm(activation, w_two)).astype(bf16)
        return four(partial), (kept, pre_act)

    def branch_backward(up, layer, stored):
        kept, pre_act = stored
        w_qkv, w_one, w_dense, w_two = layer[-1]
        grad_pre = settled(gelu_grad(pre_act, mm(up, w_two, ((1,), (1,)))).astype(bf16))
        grad_att = mm(up, w_dense, ((1,), (1,))).astype(bf16)
        pieces = attention_call(
            functools.partial(attention_backward_kernel, False),
            kept + [grad_att], tables, allowed, 3, 0,
        )
        grad_normed = mm(grad_pre, w_one, ((1,), (1,)))
        for which in range(3):
            grad_normed = grad_normed + mm(pieces[which], w_qkv[which], ((1,), (1,)))
        return four(grad_normed.astype(bf16))

    partial, stored_0 = branch_forward(flat(first_normed), layers[0])
    out_0, normed = sum_call(
        forward_kernel, n, False, 0,
        [partial, x_rows, layers[0][2], layers[1][0], layers[1][1]],
        [rows_out, full_out], rows_shape,
    )
    normed, early = settled((normed, early))
    partial, stored_1 = branch_forward(flat(normed), layers[1])
    (out_1,) = sum_call(
        forward_kernel, n, True, 1, [partial, out_0, layers[1][2]], [rows_out], rows_shape
    )
    partial = branch_backward(flat(top), layers[1], stored_1)
    grad_1, gain_1, shift_1, up = sum_call(
        backward_kernel, n, False, 2, [partial, four(top), out_0, layers[1][0]],
        [rows_out, line, line, full_out], rows_shape,
    )
    own = lambda x: lax.dynamic_index_in_dim(x, lax.axis_index("tensor"), 1, keepdims=False)
    late = gather(jnp.where(is_first, grad_1, own(normed)))
    partial = branch_backward(flat(up), layers[0], stored_0)
    grad_0, gain_0, shift_0 = sum_call(
        backward_kernel, n, True, 3, [partial, up, x_rows, layers[0][0]],
        [rows_out, line, line], rows_shape,
    )
    gain_sum = jnp.where(is_first, gain_0, gain_1)
    shift_sum = jnp.where(is_first, shift_0, shift_1)
    cut = lambda x, i: x[i * group : (i + 1) * group]

    column = lax.axis_index("dp") * (width // n_dp)
    slice_of = lambda x: lax.dynamic_slice_in_dim(x, column, width // n_dp, 1)
    total = None
    for index in range(count):
        now, then = cut(early, index), cut(late, index)
        blocks = group * n_dp
        normed_all = settled(jnp.where(is_first, now, then).reshape(blocks * rows, width))
        up_all = settled(jnp.where(is_first, then, now).reshape(blocks * rows, width))
        segment = all_segments[:, index * group : (index + 1) * group]
        segment = jnp.swapaxes(segment, 0, 1).reshape(blocks, rows)
        tables, allowed = rotary_tables(segment), allowed_of(segment)
        grad_att = mm(up_all, proj_dense, ((1,), (1,))).astype(bf16)
        *pieces, attended, s_q, s_v = attention_call(
            functools.partial(attention_backward_kernel, True),
            projections(normed_all, proj_qkv, bias_qv) + [grad_att], tables, allowed, 4, 2,
        )
        pre_act = mm(normed_all, fc_one) + bias_fc
        activation = settled(jax.nn.gelu(pre_act, approximate=True).astype(bf16))
        grad_pre = gelu_grad(pre_act, mm(up_all, fc_two, ((1,), (1,))))
        grad_fc_bias = jnp.sum(grad_pre, axis=0)
        grad_pre, grad_fc_bias = settled((grad_pre.astype(bf16), grad_fc_bias))
        normed_part, up_part = slice_of(normed_all), slice_of(up_all)
        inner = ((0,), (0,))
        terms = [mm(normed_part, p, inner) for p in pieces] + [
            mm(attended, up_part, inner),
            mm(normed_part, grad_pre, inner),
            mm(activation, up_part, inner),
            s_q[0],
            s_v[0],
            jnp.sum(up_all.astype(f32), axis=0),
            grad_fc_bias,
        ]
        total = terms if total is None else [a + b for a, b in zip(total, terms)]
    g_q, g_k, g_v, grad_dense, grad_fc_one, grad_fc_two, s_q, s_v, grad_out, grad_fc_bias = total
    norms = small_exchange(
        jnp.concatenate([gain_sum, shift_sum], axis=0), ("dp", "tensor"), 4, True
    )

    layer_out = jnp.where(is_first, out_0, out_1)
    in_grad = jnp.where(is_first, grad_0, grad_1)
    return (
        layer_out[None],
        in_grad[None],
        norms[:1],
        norms[1:],
        jnp.stack([g_q, g_k, g_v])[None],
        jnp.stack([s_q, s_v])[None],
        grad_dense[None],
        grad_out[None],
        grad_fc_one[None],
        grad_fc_bias[None],
        grad_fc_two[None],
    )


def solution(mesh):
    return jax.shard_map(
        per_device,
        mesh=mesh,
        in_specs=(
            P(None, "dp", None),
            P(None, "dp", None),
            P(None, "dp"),
            P("section", None),
            P("section", None),
            P("section", None, None, "tensor"),
            P("section", None, "tensor"),
            P("section", "tensor", None),
            P("section", None),
            P("section", None, "tensor"),
            P("section", "tensor"),
            P("section", "tensor", None),
        ),
        out_specs=(
            P("section", None, ("dp", "tensor"), None),
            P("section", None, ("dp", "tensor"), None),
            P("section", None),
            P("section", None),
            P("section", None, "dp", "tensor"),
            P("section", None, "tensor"),
            P("section", "tensor", "dp"),
            P("section", None),
            P("section", "dp", "tensor"),
            P("section", "tensor"),
            P("section", "tensor", "dp"),
        ),
        check_vma=False,
    )
```

```python
import functools

import jax
import jax.numpy as jnp
from jax import lax
from jax.experimental import pallas as pl
from jax.experimental.pallas import tpu as pltpu
from jax.sharding import PartitionSpec as P

HEAD_DIM = 64
ROT = 32

NORM_EPS = 1e-05
MASKED = -1e30
MESH = pl.DeviceIdType.MESH


def rotary_tables(segment):
    blocks, length = segment.shape
    row_index = jnp.arange(length, dtype=jnp.int32)[None, :]
    previous = jnp.concatenate([segment[:, :1], segment[:, :-1]], axis=1)
    starts = jnp.where((row_index == 0) | (segment != previous), row_index, 0)
    position = (row_index - lax.cummax(starts, axis=1)).astype(jnp.float32)
    half_rot = ROT // 2
    frequency = 10000.0 ** (-2.0 * jnp.arange(half_rot, dtype=jnp.float32) / ROT)
    phase_angle = position[..., None] * frequency
    cos_part, sin_part = jnp.cos(phase_angle), jnp.sin(phase_angle)
    none = jnp.zeros((blocks, length, half_rot), jnp.float32)
    rest = jnp.ones((blocks, length, HEAD_DIM - ROT), jnp.float32)
    straight = jnp.concatenate([cos_part, cos_part, rest], axis=-1)
    from_upper = jnp.concatenate([-sin_part, none, 0.0 * rest], axis=-1)
    from_lower = jnp.concatenate([none, sin_part, 0.0 * rest], axis=-1)
    tables = jnp.stack([straight, from_upper, from_lower], axis=1)
    return jnp.concatenate([tables, tables], axis=-1)


def allowed_of(segment):
    length = segment.shape[-1]
    row_index = jnp.arange(length, dtype=jnp.int32)
    allowed = (segment[:, :, None] == segment[:, None, :]) & (
        row_index[None, :] <= row_index[:, None]
    )
    return allowed.astype(jnp.float32)


def mm(left, right, dims=((1,), (0,))):
    return lax.dot_general(left, right, (dims, ((), ())), preferred_element_type=jnp.float32)


def rotated(x, table, sign):
    half, lanes = ROT // 2, x.shape[-1]
    return (
        x * table[0]
        + pltpu.roll(x, lanes - half, 1) * (sign * table[1])
        + pltpu.roll(x, half, 1) * (sign * table[2])
    )


def softmax_of(query, key, allowed):
    scores = mm(query, key, ((1,), (1,))) * HEAD_DIM ** (-0.5)
    scores = jnp.where(allowed, scores, MASKED)
    exps = jnp.exp(scores - jnp.max(scores, axis=-1, keepdims=True))
    return exps * (1.0 / jnp.sum(exps, axis=-1, keepdims=True))


def stacked_heads(x):
    lane = lax.broadcasted_iota(jnp.int32, (1, x.shape[-1]), 1) // HEAD_DIM
    return jnp.concatenate(
        [
            x * jnp.where(lane == h, 1.0, 0.0).astype(x.dtype)
            for h in range(x.shape[-1] // HEAD_DIM)
        ],
        axis=0,
    )


def side_by_side(x, rows):
    lane = lax.broadcasted_iota(jnp.int32, (1, x.shape[-1]), 1) // HEAD_DIM
    out = x[:rows]
    for h in range(1, x.shape[0] // rows):
        out = jnp.where(lane == h, x[h * rows : (h + 1) * rows], out)
    return out


def attention_forward_kernel(qf_ref, kf_ref, vf_ref, table_ref, allowed_ref, q_ref, k_ref, v_ref, out_ref):
    bf16 = jnp.bfloat16
    table = table_ref[0]
    rows, lanes = table.shape[-2:]
    allowed = jnp.concatenate([allowed_ref[0] > 0.5] * (lanes // HEAD_DIM), axis=0)
    for pair in range(qf_ref.shape[-1] // lanes):
        at = slice(pair * lanes, (pair + 1) * lanes)
        query = rotated(qf_ref[:, at], table, 1.0).astype(bf16)
        key = rotated(kf_ref[:, at], table, 1.0).astype(bf16)
        value = vf_ref[:, at].astype(bf16)
        q_ref[:, at] = query
        k_ref[:, at] = key
        v_ref[:, at] = value
        prob = softmax_of(stacked_heads(query), key, allowed).astype(bf16)
        out_ref[:, at] = side_by_side(mm(prob, value), rows).astype(bf16)


def attention_backward_kernel(again, q_ref, k_ref, v_ref, ga_ref, table_ref, allowed_ref, *outs):
    bf16 = jnp.bfloat16
    table = table_ref[0]
    rows, lanes = table.shape[-2:]
    allowed = jnp.concatenate([allowed_ref[0] > 0.5] * (lanes // HEAD_DIM), axis=0)
    scale = HEAD_DIM ** (-0.5)
    if again:
        gq_ref, gk_ref, gv_ref, out_ref, sq_ref, sv_ref = outs

        @pl.when(pl.program_id(0) == 0)
        def _():
            sq_ref[...] = jnp.zeros_like(sq_ref)
            sv_ref[...] = jnp.zeros_like(sv_ref)
    else:
        gq_ref, gk_ref, gv_ref = outs
    for pair in range(q_ref.shape[-1] // lanes):
        at = slice(pair * lanes, (pair + 1) * lanes)
        if again:
            query = rotated(q_ref[:, at], table, 1.0).astype(bf16)
            key = rotated(k_ref[:, at], table, 1.0).astype(bf16)
            value = v_ref[:, at].astype(bf16)
        else:
            query, key, value = q_ref[:, at], k_ref[:, at], v_ref[:, at]
        queries = stacked_heads(query)
        grads = stacked_heads(ga_ref[:, at])
        prob_f = softmax_of(queries, key, allowed)
        prob_b = prob_f.astype(bf16)
        grad_prob = mm(grads, value, ((1,), (1,)))
        row_dot = jnp.sum(prob_f * grad_prob, axis=-1, keepdims=True)
        grad_score = (prob_f * (grad_prob - row_dot)).astype(bf16)
        g_query = side_by_side(mm(grad_score, key), rows)
        g_key = mm(grad_score, queries, ((0,), (0,)))
        g_value = mm(prob_b, grads, ((0,), (0,)))
        g_query = rotated(g_query * scale, table, -1.0)
        g_key = rotated(g_key * scale, table, -1.0)
        gq_ref[:, at] = g_query.astype(bf16)
        gk_ref[:, at] = g_key.astype(bf16)
        gv_ref[:, at] = g_value.astype(bf16)
        if again:
            out_ref[:, at] = side_by_side(mm(prob_b, value), rows).astype(bf16)
            sq_ref[:, at] += jnp.sum(g_query, axis=0, keepdims=True)
            sv_ref[:, at] += jnp.sum(g_value, axis=0, keepdims=True)


def attention_call(kernel, arrays, tables, allowed, outs, sums):
    blocks, _, rows, lanes = tables.shape
    features = arrays[0].shape[-1]
    block = pl.BlockSpec((rows, features), lambda i: (i, 0))
    one = pl.BlockSpec((1, features), lambda i: (0, 0))
    flat = (blocks * rows, features)
    return pl.pallas_call(
        kernel,
        grid=(blocks,),
        in_specs=[block] * len(arrays)
        + [
            pl.BlockSpec((1, 3, rows, lanes), lambda i: (i, 0, 0, 0)),
            pl.BlockSpec((1, rows, rows), lambda i: (i, 0, 0)),
        ],
        out_specs=[block] * outs + [one] * sums,
        out_shape=[jax.ShapeDtypeStruct(flat, jnp.bfloat16)] * outs
        + [jax.ShapeDtypeStruct((1, features), jnp.float32)] * sums,
        cost_estimate=pl.CostEstimate(
            flops=20 * blocks * rows * rows * features,
            bytes_accessed=blocks * rows * features * 16,
            transcendentals=0,
        ),
    )(*arrays, tables, allowed)


def projections(normed, proj_qkv, bias_qv):
    return [
        mm(normed, proj_qkv[0]) + bias_qv[0],
        mm(normed, proj_qkv[1]),
        mm(normed, proj_qkv[2]) + bias_qv[1],
    ]


def settled(x):
    return lax.optimization_barrier(x)


def gelu_grad(pre_act, grad_act):
    _, pull_back = jax.vjp(lambda value_in: jax.nn.gelu(value_in, approximate=True), pre_act)
    return pull_back(grad_act)[0]


def normalize(hidden, norm_gain, norm_shift):
    residual = hidden.astype(jnp.float32)
    centred = residual - jnp.mean(residual, axis=-1, keepdims=True)
    inv_std = lax.rsqrt(jnp.mean(centred * centred, axis=-1, keepdims=True) + NORM_EPS)
    return (centred * inv_std * norm_gain + norm_shift).astype(jnp.bfloat16)


def partner(t, k):
    out, bit = t, 1
    while bit <= k:
        if k & bit:
            out = out + (1 - 2 * (lax.rem(lax.div(t, bit), 2))) * bit
        bit *= 2
    return out


def enter(n):
    t, sec = lax.axis_index("tensor"), lax.axis_index("section")
    barrier = pltpu.get_barrier_semaphore()
    for k in range(1, n):
        pl.semaphore_signal(
            barrier, inc=1, device_id={"tensor": partner(t, k)}, device_id_type=MESH
        )
    pl.semaphore_signal(barrier, inc=1, device_id={"section": 1 - sec}, device_id_type=MESH)
    pl.semaphore_wait(barrier, n)


def send(src, dst, sems, device):
    copy = pltpu.make_async_remote_copy(
        src_ref=src, dst_ref=dst, send_sem=sems[0], recv_sem=sems[1],
        device_id=device, device_id_type=MESH,
    )
    copy.start()
    return copy


def halves_of(width):
    sec = lax.axis_index("section")
    half = width // 2
    return (
        pl.ds(pl.multiple_of(sec * half, half), half),
        pl.ds(pl.multiple_of((1 - sec) * half, half), half),
    )


def reduced_half(n, partial_ref, scratch):
    pair, out_buf, recv, pair_sems, rs_sems = scratch
    t, sec = lax.axis_index("tensor"), lax.axis_index("section")
    mine, other = halves_of(partial_ref.shape[-1])
    enter(n)
    order = list(range(n - 1, -1, -1))
    swaps = {}
    for k in order:
        at = partner(t, k)
        swaps[k] = send(
            partial_ref.at[:, at, :, other], pair.at[k],
            [x.at[k] for x in pair_sems], {"section": 1 - sec},
        )
    sends = []
    for k in order:
        at = partner(t, k)
        swaps[k].wait_recv()
        both = partial_ref[:, at, :, mine].astype(jnp.float32) + pair[k].astype(jnp.float32)
        if k == 0:
            total = both
        else:
            out_buf[k - 1] = both.astype(jnp.bfloat16)
            sends.append(
                (k, send(out_buf.at[k - 1], recv.at[k - 1],
                         [x.at[k - 1] for x in rs_sems], {"tensor": at}))
            )
    for k, copy in sends:
        copy.wait_recv()
        total = total + recv[k - 1].astype(jnp.float32)
    return total, list(swaps.values()) + [copy for _, copy in sends]


def spread(n, full_ref, ag_sems, fw_sems):
    t, sec = lax.axis_index("tensor"), lax.axis_index("section")
    mine, _ = halves_of(full_ref.shape[-1])
    own = full_ref.at[:, t, :, mine]
    copies = [
        send(own, own, [x.at[k - 1] for x in ag_sems], {"tensor": partner(t, k)})
        for k in range(n - 1, 0, -1)
    ]
    passed = []
    for k, copy in zip(range(n - 1, 0, -1), copies):
        copy.wait_recv()
        part = full_ref.at[:, partner(t, k), :, mine]
        passed.append(send(part, part, [x.at[k - 1] for x in fw_sems], {"section": 1 - sec}))
    for copy in copies:
        copy.wait_send()
    for copy in passed:
        copy.wait()


def standard_of(rows):
    centred = rows - jnp.mean(rows, axis=-1, keepdims=True)
    inv_std = lax.rsqrt(jnp.mean(centred * centred, axis=-1, keepdims=True) + NORM_EPS)
    return centred * inv_std, inv_std


def forward_kernel(n, last, partial_ref, resid_ref, bias_ref, *rest):
    if last:
        out_ref, *scratch = rest
    else:
        gain_ref, shift_ref, out_ref, full_ref, *scratch = rest
    t, sec = lax.axis_index("tensor"), lax.axis_index("section")
    mine, _ = halves_of(partial_ref.shape[-1])
    total, copies = reduced_half(n, partial_ref, unpack(scratch))
    total = total + resid_ref[:, :, mine].astype(jnp.float32) + bias_ref[:, mine][None]
    out_ref[:, :, mine] = total.astype(jnp.bfloat16)
    part = out_ref.at[:, :, mine]
    hop = send(part, part, scratch[7:9], {"section": 1 - sec})
    hop.wait()
    if not last:
        standard, _ = standard_of(out_ref[...].astype(jnp.float32))
        full_ref[:, t] = (standard * gain_ref[...][None] + shift_ref[...][None]).astype(
            jnp.bfloat16
        )
        spread(n, full_ref, scratch[9:11], scratch[11:13])
    for copy in copies:
        copy.wait_send()


def unpack(scratch):
    pair, out_buf, recv, pair_s, pair_r, rs_s, rs_r = scratch[:7]
    return pair, out_buf, recv, (pair_s, pair_r), (rs_s, rs_r)


def backward_kernel(n, last, partial_ref, up_ref, hidden_ref, gain_ref, *rest):
    if last:
        out_ref, ggain_ref, gshift_ref, *scratch = rest
    else:
        out_ref, ggain_ref, gshift_ref, full_ref, *scratch = rest
    *scratch, whole = scratch
    t, sec = lax.axis_index("tensor"), lax.axis_index("section")
    mine, _ = halves_of(partial_ref.shape[-1])
    total, copies = reduced_half(n, partial_ref, unpack(scratch))
    whole[:, :, mine] = total
    part = whole.at[:, :, mine]
    hop = send(part, part, scratch[7:9], {"section": 1 - sec})
    standard, inv_std = standard_of(hidden_ref[...].astype(jnp.float32))
    hop.wait()
    grad_normed = whole[...]
    scaled = grad_normed * gain_ref[...][None]
    grad_in = inv_std * (
        scaled
        - jnp.mean(scaled, axis=-1, keepdims=True)
        - standard * jnp.mean(scaled * standard, axis=-1, keepdims=True)
    )
    out_ref[...] = (up_ref[:, t].astype(jnp.float32) + grad_in).astype(jnp.bfloat16)
    if not last:
        full_ref[:, t] = out_ref[...]
        spread(n, full_ref, scratch[9:11], scratch[11:13])
    ggain_ref[...] = jnp.sum(jnp.sum(grad_normed * standard, axis=0), axis=0, keepdims=True)
    gshift_ref[...] = jnp.sum(jnp.sum(grad_normed, axis=0), axis=0, keepdims=True)
    for copy in copies:
        copy.wait_send()


def sum_call(kernel, n, last, ident, args, outs, rows_shape):
    dma = pltpu.SemaphoreType.DMA
    half = rows_shape[:-1] + (rows_shape[-1] // 2,)
    scratch = [
        pltpu.VMEM((n,) + half, jnp.bfloat16),
        pltpu.VMEM((n - 1,) + half, jnp.bfloat16),
        pltpu.VMEM((n - 1,) + half, jnp.bfloat16),
        dma((n,)), dma((n,)), dma((n - 1,)), dma((n - 1,)), dma, dma,
    ]
    if not last:
        scratch += [dma((n - 1,))] * 4
    if kernel is backward_kernel:
        scratch.append(pltpu.VMEM(rows_shape, jnp.float32))
    vmem = pl.BlockSpec(memory_space=pltpu.VMEM)
    return pl.pallas_call(
        functools.partial(kernel, n, last),
        out_shape=outs,
        in_specs=[vmem] * len(args),
        out_specs=[vmem] * len(outs),
        scratch_shapes=scratch,
        compiler_params=pltpu.CompilerParams(
            collective_id=ident, has_side_effects=True, vmem_limit_bytes=32 * 1024 * 1024
        ),
    )(*args)


def exchange_kernel(axes, add, x_ref, out_ref, *rest):
    gathered, send_sem, recv_sem = rest if add else (out_ref,) + rest
    sizes = [lax.axis_size(a) for a in axes]
    index = [lax.axis_index(a) for a in axes]
    count = 1
    mine = 0
    for s, i in zip(sizes, index):
        count *= s
        mine = mine * s + i

    def shifted(k):
        ids = {}
        for a, s, i in zip(reversed(axes), reversed(sizes), reversed(index)):
            ids[a] = lax.rem(i + k % s, s)
            k //= s
        return ids

    barrier = pltpu.get_barrier_semaphore()
    for k in range(1, count):
        pl.semaphore_signal(barrier, inc=1, device_id=shifted(k), device_id_type=MESH)
    pl.semaphore_wait(barrier, count - 1)
    copies = []
    for k in range(1, count):
        copy = pltpu.make_async_remote_copy(
            src_ref=x_ref,
            dst_ref=gathered.at[mine],
            send_sem=send_sem.at[k],
            recv_sem=recv_sem.at[k],
            device_id=shifted(k),
            device_id_type=MESH,
        )
        copy.start()
        copies.append(copy)
    gathered[mine] = x_ref[...]
    for copy in copies:
        copy.wait()
    if add:
        total = gathered[0]
        for i in range(1, count):
            total = total + gathered[i]
        out_ref[...] = total


def small_exchange(x, axes, ident, add):
    count = 1
    for a in axes:
        count *= lax.axis_size(a)
    vmem = pl.BlockSpec(memory_space=pltpu.VMEM)
    stacked = (count,) + x.shape
    return pl.pallas_call(
        functools.partial(exchange_kernel, axes, add),
        out_shape=jax.ShapeDtypeStruct(x.shape if add else stacked, x.dtype),
        in_specs=[vmem],
        out_specs=vmem,
        scratch_shapes=([pltpu.VMEM(stacked, x.dtype)] if add else [])
        + [pltpu.SemaphoreType.DMA((count,)), pltpu.SemaphoreType.DMA((count,))],
        compiler_params=pltpu.CompilerParams(collective_id=ident, has_side_effects=True),
    )(x)


def per_device(
    block_input,
    cotangent,
    segments,
    ln_gain,
    ln_bias,
    qkv_weight,
    qv_bias,
    dense_weight,
    out_bias,
    fc1_weight,
    fc1_bias,
    fc2_weight,
):
    micro, rows, width = block_input.shape
    n = lax.axis_size("tensor")
    n_dp = lax.axis_size("dp")
    share = rows // n
    group = micro
    count = micro // group
    sec = lax.axis_index("section")
    is_first = sec == 0
    row_start = lax.axis_index("tensor") * share
    proj_qkv, proj_dense, fc_one, fc_two = (
        qkv_weight[0], dense_weight[0], fc1_weight[0], fc2_weight[0]
    )
    bias_qv, bias_fc = qv_bias[0], fc1_bias[0]
    bf16, f32 = jnp.bfloat16, jnp.float32
    features, hidden_units = proj_qkv.shape[-1], fc_one.shape[-1]

    swap = lambda x: lax.ppermute(x, "section", [(0, 1), (1, 0)])

    def half(x, axis, which):
        size = x.shape[axis] // 2
        return lax.dynamic_slice_in_dim(x, which * size, size, axis)

    def both(x, axis):
        return half(x, axis, sec), swap(half(x, axis, 1 - sec))

    def of_layer(index, pair):
        return jnp.where(sec == index, pair[0], pair[1])

    small = jnp.concatenate(
        [ln_gain[0], ln_bias[0], out_bias[0], bias_qv.reshape(-1), bias_fc]
    )[None]
    small_pair = (small, swap(small))
    weight_pairs = [
        both(proj_qkv, 2), both(fc_one, 1), both(proj_dense, 0), both(fc_two, 0)
    ]

    def parameters(index):
        vector = of_layer(index, small_pair)[0]
        gain, shift, bias = [vector[None, i * width : (i + 1) * width] for i in range(3)]
        at = 3 * width
        b_qv = half(vector[at : at + 2 * features].reshape(2, features), 1, sec)
        b_fc = half(vector[at + 2 * features :], 0, sec)
        return gain, shift, bias, b_qv, b_fc, [of_layer(index, p) for p in weight_pairs]

    layers = [parameters(0), parameters(1)]

    live = (segments >= 0)[:, :, None].astype(bf16)
    top = cotangent * live
    own_rows = lambda x: lax.dynamic_slice_in_dim(x, row_start, share, 1)
    first_normed = normalize(block_input, layers[0][0], layers[0][1])
    x_rows = own_rows(block_input)
    all_segments = small_exchange(segments, ("dp",), 5, False)
    tables, allowed = rotary_tables(segments), allowed_of(segments)

    def gather(x):
        return lax.all_gather(x, ("dp", "tensor"), axis=1, tiled=True)

    early = lax.all_gather(
        jnp.where(is_first, first_normed, top), "dp", axis=1, tiled=True
    )

    four = lambda x: x.reshape(micro, n, share, width)
    flat = lambda x: x.reshape(micro * rows, width)
    sds = jax.ShapeDtypeStruct
    rows_shape = (micro, share, width)
    rows_out, full_out = sds(rows_shape, bf16), sds((micro, n, share, width), bf16)
    line = sds((1, width), f32)

    def branch_forward(normed, layer):
        _, _, _, b_qv, b_fc, (w_qkv, w_one, w_dense, w_two) = layer
        *kept, attended = attention_call(
            attention_forward_kernel, projections(normed, w_qkv, b_qv), tables, allowed, 4, 0,
        )
        pre_act = mm(normed, w_one) + b_fc
        activation = settled(jax.nn.gelu(pre_act, approximate=True).astype(bf16))
        partial = (mm(attended, w_dense) + mm(activation, w_two)).astype(bf16)
        return four(partial), (kept, pre_act)

    def branch_backward(up, layer, stored):
        kept, pre_act = stored
        w_qkv, w_one, w_dense, w_two = layer[-1]
        grad_pre = settled(gelu_grad(pre_act, mm(up, w_two, ((1,), (1,)))).astype(bf16))
        grad_att = mm(up, w_dense, ((1,), (1,))).astype(bf16)
        pieces = attention_call(
            functools.partial(attention_backward_kernel, False),
            kept + [grad_att], tables, allowed, 3, 0,
        )
        grad_normed = mm(grad_pre, w_one, ((1,), (1,)))
        for which in range(3):
            grad_normed = grad_normed + mm(pieces[which], w_qkv[which], ((1,), (1,)))
        return four(grad_normed.astype(bf16))

    partial, stored_0 = branch_forward(flat(first_normed), layers[0])
    out_0, normed = sum_call(
        forward_kernel, n, False, 0,
        [partial, x_rows, layers[0][2], layers[1][0], layers[1][1]],
        [rows_out, full_out], rows_shape,
    )
    partial, stored_1 = branch_forward(flat(normed), layers[1])
    (out_1,) = sum_call(
        forward_kernel, n, True, 1, [partial, out_0, layers[1][2]], [rows_out], rows_shape
    )
    partial = branch_backward(flat(top), layers[1], stored_1)
    grad_1, gain_1, shift_1, up = sum_call(
        backward_kernel, n, False, 2, [partial, four(top), out_0, layers[1][0]],
        [rows_out, line, line, full_out], rows_shape,
    )
    own = lambda x: lax.dynamic_index_in_dim(x, lax.axis_index("tensor"), 1, keepdims=False)
    late_rows = jnp.where(is_first, grad_1, own(normed))
    up, late_rows, early = settled((up, late_rows, early))
    late = gather(late_rows)
    partial = branch_backward(flat(up), layers[0], stored_0)
    grad_0, gain_0, shift_0 = sum_call(
        backward_kernel, n, True, 3, [partial, up, x_rows, layers[0][0]],
        [rows_out, line, line], rows_shape,
    )
    gain_sum = jnp.where(is_first, gain_0, gain_1)
    shift_sum = jnp.where(is_first, shift_0, shift_1)
    cut = lambda x, i: x[i * group : (i + 1) * group]

    column = lax.axis_index("dp") * (width // n_dp)
    slice_of = lambda x: lax.dynamic_slice_in_dim(x, column, width // n_dp, 1)
    total = None
    for index in range(count):
        now, then = cut(early, index), cut(late, index)
        blocks = group * n_dp
        normed_all = settled(jnp.where(is_first, now, then).reshape(blocks * rows, width))
        up_all = settled(jnp.where(is_first, then, now).reshape(blocks * rows, width))
        segment = all_segments[:, index * group : (index + 1) * group]
        segment = jnp.swapaxes(segment, 0, 1).reshape(blocks, rows)
        tables, allowed = rotary_tables(segment), allowed_of(segment)
        grad_att = mm(up_all, proj_dense, ((1,), (1,))).astype(bf16)
        *pieces, attended, s_q, s_v = attention_call(
            functools.partial(attention_backward_kernel, True),
            projections(normed_all, proj_qkv, bias_qv) + [grad_att], tables, allowed, 4, 2,
        )
        pre_act = mm(normed_all, fc_one) + bias_fc
        activation = settled(jax.nn.gelu(pre_act, approximate=True).astype(bf16))
        grad_pre = gelu_grad(pre_act, mm(up_all, fc_two, ((1,), (1,))))
        grad_fc_bias = jnp.sum(grad_pre, axis=0)
        grad_pre, grad_fc_bias = settled((grad_pre.astype(bf16), grad_fc_bias))
        normed_part, up_part = slice_of(normed_all), slice_of(up_all)
        inner = ((0,), (0,))
        terms = [mm(normed_part, p, inner) for p in pieces] + [
            mm(attended, up_part, inner),
            mm(normed_part, grad_pre, inner),
            mm(activation, up_part, inner),
            s_q[0],
            s_v[0],
            jnp.sum(up_all.astype(f32), axis=0),
            grad_fc_bias,
        ]
        total = terms if total is None else [a + b for a, b in zip(total, terms)]
    g_q, g_k, g_v, grad_dense, grad_fc_one, grad_fc_two, s_q, s_v, grad_out, grad_fc_bias = total
    norms = small_exchange(
        jnp.concatenate([gain_sum, shift_sum], axis=0), ("dp", "tensor"), 4, True
    )

    layer_out = jnp.where(is_first, out_0, out_1)
    in_grad = jnp.where(is_first, grad_0, grad_1)
    return (
        layer_out[None],
        in_grad[None],
        norms[:1],
        norms[1:],
        jnp.stack([g_q, g_k, g_v])[None],
        jnp.stack([s_q, s_v])[None],
        grad_dense[None],
        grad_out[None],
        grad_fc_one[None],
        grad_fc_bias[None],
        grad_fc_two[None],
    )


def solution(mesh):
    return jax.shard_map(
        per_device,
        mesh=mesh,
        in_specs=(
            P(None, "dp", None),
            P(None, "dp", None),
            P(None, "dp"),
            P("section", None),
            P("section", None),
            P("section", None, None, "tensor"),
            P("section", None, "tensor"),
            P("section", "tensor", None),
            P("section", None),
            P("section", None, "tensor"),
            P("section", "tensor"),
            P("section", "tensor", None),
        ),
        out_specs=(
            P("section", None, ("dp", "tensor"), None),
            P("section", None, ("dp", "tensor"), None),
            P("section", None),
            P("section", None),
            P("section", None, "dp", "tensor"),
            P("section", None, "tensor"),
            P("section", "tensor", "dp"),
            P("section", None),
            P("section", "dp", "tensor"),
            P("section", "tensor"),
            P("section", "tensor", "dp"),
        ),
        check_vma=False,
    )
```

```python
import functools

import jax
import jax.numpy as jnp
from jax import lax
from jax.experimental import pallas as pl
from jax.experimental.pallas import tpu as pltpu
from jax.sharding import PartitionSpec as P

HEAD_DIM = 64
ROT = 32

NORM_EPS = 1e-05
MASKED = -1e30
MESH = pl.DeviceIdType.MESH


def rotary_tables(segment):
    blocks, length = segment.shape
    row_index = jnp.arange(length, dtype=jnp.int32)[None, :]
    previous = jnp.concatenate([segment[:, :1], segment[:, :-1]], axis=1)
    starts = jnp.where((row_index == 0) | (segment != previous), row_index, 0)
    position = (row_index - lax.cummax(starts, axis=1)).astype(jnp.float32)
    half_rot = ROT // 2
    frequency = 10000.0 ** (-2.0 * jnp.arange(half_rot, dtype=jnp.float32) / ROT)
    phase_angle = position[..., None] * frequency
    cos_part, sin_part = jnp.cos(phase_angle), jnp.sin(phase_angle)
    none = jnp.zeros((blocks, length, half_rot), jnp.float32)
    rest = jnp.ones((blocks, length, HEAD_DIM - ROT), jnp.float32)
    straight = jnp.concatenate([cos_part, cos_part, rest], axis=-1)
    from_upper = jnp.concatenate([-sin_part, none, 0.0 * rest], axis=-1)
    from_lower = jnp.concatenate([none, sin_part, 0.0 * rest], axis=-1)
    tables = jnp.stack([straight, from_upper, from_lower], axis=1)
    return jnp.concatenate([tables, tables], axis=-1)


def allowed_of(segment):
    length = segment.shape[-1]
    row_index = jnp.arange(length, dtype=jnp.int32)
    allowed = (segment[:, :, None] == segment[:, None, :]) & (
        row_index[None, :] <= row_index[:, None]
    )
    return allowed.astype(jnp.float32)


def mm(left, right, dims=((1,), (0,))):
    return lax.dot_general(left, right, (dims, ((), ())), preferred_element_type=jnp.float32)


def rotated(x, table, sign):
    half, lanes = ROT // 2, x.shape[-1]
    return (
        x * table[0]
        + pltpu.roll(x, lanes - half, 1) * (sign * table[1])
        + pltpu.roll(x, half, 1) * (sign * table[2])
    )


def softmax_of(query, key, allowed):
    scores = mm(query, key, ((1,), (1,))) * HEAD_DIM ** (-0.5)
    scores = jnp.where(allowed, scores, MASKED)
    exps = jnp.exp(scores - jnp.max(scores, axis=-1, keepdims=True))
    return exps * (1.0 / jnp.sum(exps, axis=-1, keepdims=True))


def stacked_heads(x):
    lane = lax.broadcasted_iota(jnp.int32, (1, x.shape[-1]), 1) // HEAD_DIM
    return jnp.concatenate(
        [
            x * jnp.where(lane == h, 1.0, 0.0).astype(x.dtype)
            for h in range(x.shape[-1] // HEAD_DIM)
        ],
        axis=0,
    )


def side_by_side(x, rows):
    lane = lax.broadcasted_iota(jnp.int32, (1, x.shape[-1]), 1) // HEAD_DIM
    out = x[:rows]
    for h in range(1, x.shape[0] // rows):
        out = jnp.where(lane == h, x[h * rows : (h + 1) * rows], out)
    return out


def attention_forward_kernel(qf_ref, kf_ref, vf_ref, table_ref, allowed_ref, q_ref, k_ref, v_ref, out_ref):
    bf16 = jnp.bfloat16
    table = table_ref[0]
    rows, lanes = table.shape[-2:]
    allowed = jnp.concatenate([allowed_ref[0] > 0.5] * (lanes // HEAD_DIM), axis=0)
    for pair in range(qf_ref.shape[-1] // lanes):
        at = slice(pair * lanes, (pair + 1) * lanes)
        query = rotated(qf_ref[:, at], table, 1.0).astype(bf16)
        key = rotated(kf_ref[:, at], table, 1.0).astype(bf16)
        value = vf_ref[:, at].astype(bf16)
        q_ref[:, at] = query
        k_ref[:, at] = key
        v_ref[:, at] = value
        prob = softmax_of(stacked_heads(query), key, allowed).astype(bf16)
        out_ref[:, at] = side_by_side(mm(prob, value), rows).astype(bf16)


def pair_backward(query, key, value, grad, table, allowed, with_output):
    bf16 = jnp.bfloat16
    rows, scale = query.shape[0], HEAD_DIM ** (-0.5)
    queries, grads = stacked_heads(query), stacked_heads(grad)
    prob_f = softmax_of(queries, key, allowed)
    prob_b = prob_f.astype(bf16)
    grad_prob = mm(grads, value, ((1,), (1,)))
    row_dot = jnp.sum(prob_f * grad_prob, axis=-1, keepdims=True)
    grad_score = (prob_f * (grad_prob - row_dot)).astype(bf16)
    g_query = side_by_side(mm(grad_score, key), rows)
    g_key = mm(grad_score, queries, ((0,), (0,)))
    g_value = mm(prob_b, grads, ((0,), (0,)))
    g_query = rotated(g_query * scale, table, -1.0)
    g_key = rotated(g_key * scale, table, -1.0)
    out = side_by_side(mm(prob_b, value), rows).astype(bf16) if with_output else None
    return g_query, g_key, g_value, out


def attention_backward_kernel(q_ref, k_ref, v_ref, ga_ref, table_ref, allowed_ref, gq_ref, gk_ref, gv_ref):
    bf16 = jnp.bfloat16
    table = table_ref[0]
    lanes = table.shape[-1]
    allowed = jnp.concatenate([allowed_ref[0] > 0.5] * (lanes // HEAD_DIM), axis=0)
    for pair in range(q_ref.shape[-1] // lanes):
        at = slice(pair * lanes, (pair + 1) * lanes)
        g_query, g_key, g_value, _ = pair_backward(
            q_ref[:, at], k_ref[:, at], v_ref[:, at], ga_ref[:, at], table, allowed, False
        )
        gq_ref[:, at] = g_query.astype(bf16)
        gk_ref[:, at] = g_key.astype(bf16)
        gv_ref[:, at] = g_value.astype(bf16)


def attention_again_kernel(
    normed_ref, up_ref, w_ref, dense_ref, bias_ref, table_ref, allowed_ref,
    gq_ref, gk_ref, gv_ref, out_ref, sq_ref, sv_ref, su_ref,
):
    bf16 = jnp.bfloat16
    count, _, rows, lanes = table_ref.shape
    features = gq_ref.shape[-1]
    wide = min(2 * lanes, features)

    @pl.when(pl.program_id(0) == 0)
    def _():
        sq_ref[...] = jnp.zeros_like(sq_ref)
        sv_ref[...] = jnp.zeros_like(sv_ref)
        su_ref[...] = jnp.zeros_like(su_ref)

    su_ref[...] += jnp.sum(up_ref[...].astype(jnp.float32), axis=0, keepdims=True)

    def products(at):
        cols = slice(at, at + wide)
        return (
            mm(normed_ref[...], w_ref[0, :, cols]) + bias_ref[0:1, cols],
            mm(normed_ref[...], w_ref[1, :, cols]),
            (mm(normed_ref[...], w_ref[2, :, cols]) + bias_ref[1:2, cols]).astype(bf16),
            mm(up_ref[...], dense_ref[cols, :], ((1,), (1,))).astype(bf16),
        )

    starts = list(range(0, features, wide))
    ready = products(starts[0])
    for index, start in enumerate(starts):
        upcoming = products(starts[index + 1]) if index + 1 < len(starts) else None
        for block in range(count):
            table = table_ref[block]
            allowed = jnp.concatenate([allowed_ref[block] > 0.5] * (lanes // HEAD_DIM), axis=0)
            down = slice(block * rows, (block + 1) * rows)
            for pair in range(wide // lanes):
                inside = slice(pair * lanes, (pair + 1) * lanes)
                query_f, key_f, value, grad = [x[down, inside] for x in ready]
                query = rotated(query_f, table, 1.0).astype(bf16)
                key = rotated(key_f, table, 1.0).astype(bf16)
                g_query, g_key, g_value, out = pair_backward(
                    query, key, value, grad, table, allowed, True
                )
                at = slice(start + pair * lanes, start + (pair + 1) * lanes)
                gq_ref[down, at] = g_query.astype(bf16)
                gk_ref[down, at] = g_key.astype(bf16)
                gv_ref[down, at] = g_value.astype(bf16)
                out_ref[down, at] = out
                sq_ref[:, at] += jnp.sum(g_query, axis=0, keepdims=True)
                sv_ref[:, at] += jnp.sum(g_value, axis=0, keepdims=True)
        ready = upcoming


def attention_again(normed, up, proj_qkv, proj_dense, bias_qv, tables, allowed):
    blocks, _, rows, lanes = tables.shape
    features, width = proj_dense.shape
    count = 2 if blocks % 2 == 0 else 1
    wide = pl.BlockSpec((count * rows, width), lambda i: (i, 0))
    block = pl.BlockSpec((count * rows, features), lambda i: (i, 0))
    one = pl.BlockSpec((1, features), lambda i: (0, 0))
    flat = jax.ShapeDtypeStruct((blocks * rows, features), jnp.bfloat16)
    line = jax.ShapeDtypeStruct((1, features), jnp.float32)
    once = pl.Buffered(1)
    return pl.pallas_call(
        attention_again_kernel,
        grid=(blocks // count,),
        in_specs=[
            wide,
            wide,
            pl.BlockSpec(proj_qkv.shape, lambda i: (0, 0, 0), pipeline_mode=once),
            pl.BlockSpec(proj_dense.shape, lambda i: (0, 0), pipeline_mode=once),
            pl.BlockSpec(bias_qv.shape, lambda i: (0, 0)),
            pl.BlockSpec((count, 3, rows, lanes), lambda i: (i, 0, 0, 0)),
            pl.BlockSpec((count, rows, rows), lambda i: (i, 0, 0)),
        ],
        out_specs=[block] * 4 + [one] * 2 + [pl.BlockSpec((1, width), lambda i: (0, 0))],
        out_shape=[flat] * 4 + [line] * 2 + [jax.ShapeDtypeStruct((1, width), jnp.float32)],
        cost_estimate=pl.CostEstimate(
            flops=8 * blocks * rows * width * features,
            bytes_accessed=blocks * rows * (width * 4 + features * 8),
            transcendentals=0,
        ),
    )(normed, up, proj_qkv, proj_dense, bias_qv, tables, allowed)


def attention_call(kernel, arrays, tables, allowed, outs):
    blocks, _, rows, lanes = tables.shape
    features = arrays[0].shape[-1]
    block = pl.BlockSpec((rows, features), lambda i: (i, 0))
    flat = (blocks * rows, features)
    return pl.pallas_call(
        kernel,
        grid=(blocks,),
        in_specs=[block] * len(arrays)
        + [
            pl.BlockSpec((1, 3, rows, lanes), lambda i: (i, 0, 0, 0)),
            pl.BlockSpec((1, rows, rows), lambda i: (i, 0, 0)),
        ],
        out_specs=[block] * outs,
        out_shape=[jax.ShapeDtypeStruct(flat, jnp.bfloat16)] * outs,
        cost_estimate=pl.CostEstimate(
            flops=20 * blocks * rows * rows * features,
            bytes_accessed=blocks * rows * features * 16,
            transcendentals=0,
        ),
    )(*arrays, tables, allowed)


def projections(normed, proj_qkv, bias_qv):
    return [
        mm(normed, proj_qkv[0]) + bias_qv[0],
        mm(normed, proj_qkv[1]),
        mm(normed, proj_qkv[2]) + bias_qv[1],
    ]


def settled(x):
    return lax.optimization_barrier(x)


def gelu_grad(pre_act, grad_act):
    _, pull_back = jax.vjp(lambda value_in: jax.nn.gelu(value_in, approximate=True), pre_act)
    return pull_back(grad_act)[0]


def normalize(hidden, norm_gain, norm_shift):
    residual = hidden.astype(jnp.float32)
    centred = residual - jnp.mean(residual, axis=-1, keepdims=True)
    inv_std = lax.rsqrt(jnp.mean(centred * centred, axis=-1, keepdims=True) + NORM_EPS)
    return (centred * inv_std * norm_gain + norm_shift).astype(jnp.bfloat16)


def partner(t, k):
    out, bit = t, 1
    while bit <= k:
        if k & bit:
            out = out + (1 - 2 * (lax.rem(lax.div(t, bit), 2))) * bit
        bit *= 2
    return out


def enter(n):
    t, sec = lax.axis_index("tensor"), lax.axis_index("section")
    barrier = pltpu.get_barrier_semaphore()
    for k in range(1, n):
        pl.semaphore_signal(
            barrier, inc=1, device_id={"tensor": partner(t, k)}, device_id_type=MESH
        )
    pl.semaphore_signal(barrier, inc=1, device_id={"section": 1 - sec}, device_id_type=MESH)
    pl.semaphore_wait(barrier, n)


def send(src, dst, sems, device):
    copy = pltpu.make_async_remote_copy(
        src_ref=src, dst_ref=dst, send_sem=sems[0], recv_sem=sems[1],
        device_id=device, device_id_type=MESH,
    )
    copy.start()
    return copy


def halves_of(width):
    sec = lax.axis_index("section")
    half = width // 2
    return (
        pl.ds(pl.multiple_of(sec * half, half), half),
        pl.ds(pl.multiple_of((1 - sec) * half, half), half),
    )


def start_swaps(n, partial_ref, scratch):
    pair, _, _, pair_sems, _ = scratch
    t, sec = lax.axis_index("tensor"), lax.axis_index("section")
    _, other = halves_of(partial_ref.shape[-1])
    return {
        k: send(
            partial_ref.at[:, partner(t, k), :, other], pair.at[k],
            [x.at[k] for x in pair_sems], {"section": 1 - sec},
        )
        for k in range(n - 1, -1, -1)
    }


def start_sums(n, partial_ref, scratch, swaps):
    pair, out_buf, recv, _, rs_sems = scratch
    t = lax.axis_index("tensor")
    mine, _ = halves_of(partial_ref.shape[-1])
    sends = []
    for k in range(n - 1, -1, -1):
        at = partner(t, k)
        swaps[k].wait_recv()
        both = partial_ref[:, at, :, mine].astype(jnp.float32) + pair[k].astype(jnp.float32)
        if k:
            out_buf[k - 1] = both.astype(jnp.bfloat16)
            sends.append(
                (k, send(out_buf.at[k - 1], recv.at[k - 1],
                         [x.at[k - 1] for x in rs_sems], {"tensor": at}))
            )
    return both, sends


def finish_sums(total, scratch, sends):
    recv = scratch[2]
    for k, copy in sends:
        copy.wait_recv()
        total = total + recv[k - 1].astype(jnp.float32)
    return total


def reduced_half(n, partial_ref, scratch):
    enter(n)
    swaps = start_swaps(n, partial_ref, scratch)
    total, sends = start_sums(n, partial_ref, scratch, swaps)
    total = finish_sums(total, scratch, sends)
    return total, list(swaps.values()) + [copy for _, copy in sends]


def spread(n, full_ref, ag_sems, fw_sems):
    t, sec = lax.axis_index("tensor"), lax.axis_index("section")
    mine, _ = halves_of(full_ref.shape[-1])
    own = full_ref.at[:, t, :, mine]
    copies = [
        send(own, own, [x.at[k - 1] for x in ag_sems], {"tensor": partner(t, k)})
        for k in range(n - 1, 0, -1)
    ]
    passed = []
    for k, copy in zip(range(n - 1, 0, -1), copies):
        copy.wait_recv()
        part = full_ref.at[:, partner(t, k), :, mine]
        passed.append(send(part, part, [x.at[k - 1] for x in fw_sems], {"section": 1 - sec}))
    for copy in copies:
        copy.wait_send()
    for copy in passed:
        copy.wait()


def standard_of(rows):
    centred = rows - jnp.mean(rows, axis=-1, keepdims=True)
    inv_std = lax.rsqrt(jnp.mean(centred * centred, axis=-1, keepdims=True) + NORM_EPS)
    return centred * inv_std, inv_std


def forward_kernel(
    n, partial_ref, resid_ref, bias_ref, gain_ref, shift_ref, out_ref, full_ref, *scratch
):
    t, sec = lax.axis_index("tensor"), lax.axis_index("section")
    mine, _ = halves_of(partial_ref.shape[-1])
    total, copies = reduced_half(n, partial_ref, unpack(scratch))
    total = total + resid_ref[:, :, mine].astype(jnp.float32) + bias_ref[:, mine][None]
    out_ref[:, :, mine] = total.astype(jnp.bfloat16)
    part = out_ref.at[:, :, mine]
    hop = send(part, part, scratch[7:9], {"section": 1 - sec})
    hop.wait()
    standard, _ = standard_of(out_ref[...].astype(jnp.float32))
    full_ref[:, t] = (standard * gain_ref[...][None] + shift_ref[...][None]).astype(jnp.bfloat16)
    spread(n, full_ref, scratch[9:11], scratch[11:13])
    for copy in copies:
        copy.wait_send()


def unpack(scratch):
    pair, out_buf, recv, pair_s, pair_r, rs_s, rs_r = scratch[:7]
    return pair, out_buf, recv, (pair_s, pair_r), (rs_s, rs_r)


def norm_backward(grad_normed, hidden_ref, gain_ref, up_rows, ggain_ref, gshift_ref):
    standard, inv_std = standard_of(hidden_ref[...].astype(jnp.float32))
    scaled = grad_normed * gain_ref[...][None]
    grad_in = inv_std * (
        scaled
        - jnp.mean(scaled, axis=-1, keepdims=True)
        - standard * jnp.mean(scaled * standard, axis=-1, keepdims=True)
    )
    ggain_ref[...] = jnp.sum(jnp.sum(grad_normed * standard, axis=0), axis=0, keepdims=True)
    gshift_ref[...] = jnp.sum(jnp.sum(grad_normed, axis=0), axis=0, keepdims=True)
    return (up_rows.astype(jnp.float32) + grad_in).astype(jnp.bfloat16)


def backward_kernel(
    n, partial_ref, up_ref, hidden_ref, gain_ref, out_ref, ggain_ref, gshift_ref, full_ref,
    whole, *scratch
):
    t, sec = lax.axis_index("tensor"), lax.axis_index("section")
    mine, _ = halves_of(partial_ref.shape[-1])
    total, copies = reduced_half(n, partial_ref, unpack(scratch))
    whole[:, :, mine] = total
    part = whole.at[:, :, mine]
    hop = send(part, part, scratch[7:9], {"section": 1 - sec})
    hop.wait()
    out_ref[...] = norm_backward(
        whole[...], hidden_ref, gain_ref, up_ref[:, t], ggain_ref, gshift_ref
    )
    full_ref[:, t] = out_ref[...]
    spread(n, full_ref, scratch[9:11], scratch[11:13])
    for copy in copies:
        copy.wait_send()


def final_kernel(
    n, partial_ref, resid_ref, bias_ref, grad_ref, up_ref, hidden_ref, gain_ref,
    out_ref, down_ref, ggain_ref, gshift_ref, whole, *scratch
):
    t, sec = lax.axis_index("tensor"), lax.axis_index("section")
    mine, _ = halves_of(partial_ref.shape[-1])
    sets = [unpack(scratch[:9]), unpack(scratch[9:])]
    hops = [scratch[7:9], scratch[16:18]]
    refs = [grad_ref, partial_ref]
    enter(n)
    swaps = [start_swaps(n, ref, x) for ref, x in zip(refs, sets)]
    sums = [start_sums(n, ref, x, w) for ref, x, w in zip(refs, sets, swaps)]
    whole[:, :, mine] = finish_sums(sums[0][0], sets[0], sums[0][1])
    part = whole.at[:, :, mine]
    first = send(part, part, hops[0], {"section": 1 - sec})
    total = finish_sums(sums[1][0], sets[1], sums[1][1])
    total = total + resid_ref[:, :, mine].astype(jnp.float32) + bias_ref[:, mine][None]
    out_ref[:, :, mine] = total.astype(jnp.bfloat16)
    part = out_ref.at[:, :, mine]
    second = send(part, part, hops[1], {"section": 1 - sec})
    first.wait()
    down_ref[...] = norm_backward(
        whole[...], hidden_ref, gain_ref, up_ref[:, t], ggain_ref, gshift_ref
    )
    second.wait()
    for w in swaps:
        for copy in w.values():
            copy.wait_send()
    for _, sends in sums:
        for _, copy in sends:
            copy.wait_send()


def sum_call(kernel, n, ident, args, outs, rows_shape):
    dma = pltpu.SemaphoreType.DMA
    half = rows_shape[:-1] + (rows_shape[-1] // 2,)
    scratch = [
        pltpu.VMEM((n,) + half, jnp.bfloat16),
        pltpu.VMEM((n - 1,) + half, jnp.bfloat16),
        pltpu.VMEM((n - 1,) + half, jnp.bfloat16),
        dma((n,)), dma((n,)), dma((n - 1,)), dma((n - 1,)), dma, dma,
    ]
    scratch += scratch if kernel is final_kernel else [dma((n - 1,))] * 4
    if kernel is not forward_kernel:
        scratch = [pltpu.VMEM(rows_shape, jnp.float32)] + scratch
    vmem = pl.BlockSpec(memory_space=pltpu.VMEM)
    return pl.pallas_call(
        functools.partial(kernel, n),
        out_shape=outs,
        in_specs=[vmem] * len(args),
        out_specs=[vmem] * len(outs),
        scratch_shapes=scratch,
        compiler_params=pltpu.CompilerParams(
            collective_id=ident, has_side_effects=True, vmem_limit_bytes=32 * 1024 * 1024
        ),
    )(*args)


GELU_A = (2.0 / jnp.pi) ** 0.5
GELU_B = 0.044715


def hidden_kernel(first, x_ref, known_ref, w_ref, b_ref, act_ref, grad_ref, sum_ref):
    @pl.when(pl.program_id(1) == 0)
    def _():
        sum_ref[...] = jnp.zeros_like(sum_ref)

    step = 256
    starts = list(range(0, act_ref.shape[-1], step))

    def product(at):
        cols = slice(at, at + step)
        if first:
            return mm(x_ref[...], w_ref[cols, :], ((1,), (1,)))
        return mm(x_ref[...], w_ref[:, cols]) + b_ref[:, cols]

    ready = product(starts[0])
    for index, at in enumerate(starts):
        cols = slice(at, at + step)
        upcoming = product(starts[index + 1]) if index + 1 < len(starts) else None
        pre, grad_act = (known_ref[:, cols], ready) if first else (ready, known_ref[:, cols])
        square = pre * pre
        bent = jnp.tanh(pre * (GELU_A + (GELU_A * GELU_B) * square))
        gate = 0.5 + 0.5 * bent
        act_ref[:, cols] = (pre * gate).astype(jnp.bfloat16)
        slope = gate + (0.5 * pre) * (1.0 - bent * bent) * (
            GELU_A + (3.0 * GELU_A * GELU_B) * square
        )
        grad_pre = grad_act * slope
        grad_ref[:, cols] = grad_pre.astype(jnp.bfloat16)
        sum_ref[:, cols] += jnp.sum(grad_pre, axis=0, keepdims=True)
        ready = upcoming


def hidden_call(first, x, known, weight, bias):
    tokens, width = x.shape
    units = known.shape[-1]
    tile, chunk = 256, min(1024, units)
    flat = pl.BlockSpec((tile, chunk), lambda j, i: (i, j))
    line = pl.BlockSpec((1, chunk), lambda j, i: (0, j))
    w_spec = (
        pl.BlockSpec((chunk, width), lambda j, i: (j, 0))
        if first
        else pl.BlockSpec((width, chunk), lambda j, i: (0, j))
    )
    out = jax.ShapeDtypeStruct((tokens, units), jnp.bfloat16)
    return pl.pallas_call(
        functools.partial(hidden_kernel, first),
        grid=(units // chunk, tokens // tile),
        in_specs=[pl.BlockSpec((tile, width), lambda j, i: (i, 0)), flat, w_spec, line],
        out_specs=[flat, flat, line],
        out_shape=[out, out, jax.ShapeDtypeStruct((1, units), jnp.float32)],
        cost_estimate=pl.CostEstimate(
            flops=2 * tokens * width * units,
            bytes_accessed=tokens * (units * 8 + width * 4),
            transcendentals=tokens * units,
        ),
    )(x, known, weight, bias[None])


def exchange_kernel(axes, add, x_ref, out_ref, *rest):
    gathered, send_sem, recv_sem = rest if add else (out_ref,) + rest
    sizes = [lax.axis_size(a) for a in axes]
    index = [lax.axis_index(a) for a in axes]
    count = 1
    mine = 0
    for s, i in zip(sizes, index):
        count *= s
        mine = mine * s + i

    def shifted(k):
        ids = {}
        for a, s, i in zip(reversed(axes), reversed(sizes), reversed(index)):
            ids[a] = lax.rem(i + k % s, s)
            k //= s
        return ids

    barrier = pltpu.get_barrier_semaphore()
    for k in range(1, count):
        pl.semaphore_signal(barrier, inc=1, device_id=shifted(k), device_id_type=MESH)
    pl.semaphore_wait(barrier, count - 1)
    copies = []
    for k in range(1, count):
        copy = pltpu.make_async_remote_copy(
            src_ref=x_ref,
            dst_ref=gathered.at[mine],
            send_sem=send_sem.at[k],
            recv_sem=recv_sem.at[k],
            device_id=shifted(k),
            device_id_type=MESH,
        )
        copy.start()
        copies.append(copy)
    gathered[mine] = x_ref[...]
    for copy in copies:
        copy.wait()
    if add:
        total = gathered[0]
        for i in range(1, count):
            total = total + gathered[i]
        out_ref[...] = total


def small_exchange(x, axes, ident, add):
    count = 1
    for a in axes:
        count *= lax.axis_size(a)
    vmem = pl.BlockSpec(memory_space=pltpu.VMEM)
    stacked = (count,) + x.shape
    return pl.pallas_call(
        functools.partial(exchange_kernel, axes, add),
        out_shape=jax.ShapeDtypeStruct(x.shape if add else stacked, x.dtype),
        in_specs=[vmem],
        out_specs=vmem,
        scratch_shapes=([pltpu.VMEM(stacked, x.dtype)] if add else [])
        + [pltpu.SemaphoreType.DMA((count,)), pltpu.SemaphoreType.DMA((count,))],
        compiler_params=pltpu.CompilerParams(collective_id=ident, has_side_effects=True),
    )(x)


def per_device(
    block_input,
    cotangent,
    segments,
    ln_gain,
    ln_bias,
    qkv_weight,
    qv_bias,
    dense_weight,
    out_bias,
    fc1_weight,
    fc1_bias,
    fc2_weight,
):
    micro, rows, width = block_input.shape
    n = lax.axis_size("tensor")
    n_dp = lax.axis_size("dp")
    share = rows // n
    sec = lax.axis_index("section")
    is_first = sec == 0
    row_start = lax.axis_index("tensor") * share
    proj_qkv, proj_dense, fc_one, fc_two = (
        qkv_weight[0], dense_weight[0], fc1_weight[0], fc2_weight[0]
    )
    bias_qv, bias_fc = qv_bias[0], fc1_bias[0]
    bf16, f32 = jnp.bfloat16, jnp.float32
    features, hidden_units = proj_qkv.shape[-1], fc_one.shape[-1]

    swap = lambda x: lax.ppermute(x, "section", [(0, 1), (1, 0)])

    def half(x, axis, which):
        size = x.shape[axis] // 2
        return lax.dynamic_slice_in_dim(x, which * size, size, axis)

    def both(x, axis):
        return half(x, axis, sec), swap(half(x, axis, 1 - sec))

    def of_layer(index, pair):
        return jnp.where(sec == index, pair[0], pair[1])

    small = jnp.concatenate(
        [ln_gain[0], ln_bias[0], out_bias[0], bias_qv.reshape(-1), bias_fc]
    )[None]
    small_pair = (small, swap(small))
    weight_pairs = [
        both(proj_qkv, 2), both(fc_one, 1), both(proj_dense, 0), both(fc_two, 0)
    ]

    def parameters(index):
        vector = of_layer(index, small_pair)[0]
        gain, shift, bias = [vector[None, i * width : (i + 1) * width] for i in range(3)]
        at = 3 * width
        b_qv = half(vector[at : at + 2 * features].reshape(2, features), 1, sec)
        b_fc = half(vector[at + 2 * features :], 0, sec)
        return gain, shift, bias, b_qv, b_fc, [of_layer(index, p) for p in weight_pairs]

    layers = [parameters(0), parameters(1)]

    live = (segments >= 0)[:, :, None].astype(bf16)
    top = cotangent * live
    own_rows = lambda x: lax.dynamic_slice_in_dim(x, row_start, share, 1)
    first_normed = normalize(block_input, layers[0][0], layers[0][1])
    x_rows = own_rows(block_input)
    all_segments = small_exchange(segments, ("dp",), 5, False)
    tables, allowed = rotary_tables(segments), allowed_of(segments)

    def gather(x):
        return lax.all_gather(x, ("dp", "tensor"), axis=1, tiled=True)

    early = lax.all_gather(
        jnp.where(is_first, first_normed, top), "dp", axis=1, tiled=True
    )

    four = lambda x: x.reshape(micro, n, share, width)
    flat = lambda x: x.reshape(micro * rows, width)
    sds = jax.ShapeDtypeStruct
    rows_shape = (micro, share, width)
    rows_out, full_out = sds(rows_shape, bf16), sds((micro, n, share, width), bf16)
    line = sds((1, width), f32)

    def branch_forward(normed, layer):
        _, _, _, b_qv, b_fc, (w_qkv, w_one, w_dense, w_two) = layer
        *kept, attended = attention_call(
            attention_forward_kernel, projections(normed, w_qkv, b_qv), tables, allowed, 4,
        )
        pre_act = mm(normed, w_one) + b_fc
        activation = settled(jax.nn.gelu(pre_act, approximate=True).astype(bf16))
        partial = (mm(attended, w_dense) + mm(activation, w_two)).astype(bf16)
        return four(partial), (kept, pre_act)

    def branch_backward(up, layer, stored):
        kept, pre_act = stored
        w_qkv, w_one, w_dense, w_two = layer[-1]
        grad_pre = settled(gelu_grad(pre_act, mm(up, w_two, ((1,), (1,)))).astype(bf16))
        grad_att = mm(up, w_dense, ((1,), (1,))).astype(bf16)
        pieces = attention_call(
            attention_backward_kernel, kept + [grad_att], tables, allowed, 3,
        )
        grad_normed = mm(grad_pre, w_one, ((1,), (1,)))
        for which in range(3):
            grad_normed = grad_normed + mm(pieces[which], w_qkv[which], ((1,), (1,)))
        return four(grad_normed.astype(bf16))

    partial, stored_0 = branch_forward(flat(first_normed), layers[0])
    out_0, normed = sum_call(
        forward_kernel, n, 0,
        [partial, x_rows, layers[0][2], layers[1][0], layers[1][1]],
        [rows_out, full_out], rows_shape,
    )
    last_partial, stored_1 = branch_forward(flat(normed), layers[1])
    partial = branch_backward(flat(top), layers[1], stored_1)
    grad_1, gain_1, shift_1, up = sum_call(
        backward_kernel, n, 2, [partial, four(top), out_0, layers[1][0]],
        [rows_out, line, line, full_out], rows_shape,
    )
    own = lambda x: lax.dynamic_index_in_dim(x, lax.axis_index("tensor"), 1, keepdims=False)
    late_rows = jnp.where(is_first, grad_1, own(normed))
    up, late_rows, early = settled((up, late_rows, early))
    late = gather(late_rows)
    partial = branch_backward(flat(up), layers[0], stored_0)

    tokens = micro * n_dp * rows
    early = early.reshape(tokens, width)
    known = lax.cond(
        is_first,
        lambda x: mm(x, fc_one) + bias_fc,
        lambda x: mm(x, fc_two, ((1,), (1,))),
        early,
    )
    partial, last_partial, known = settled((partial, last_partial, known))
    out_1, grad_0, gain_0, shift_0 = sum_call(
        final_kernel, n, 1,
        [last_partial, out_0, layers[1][2], partial, up, x_rows, layers[0][0]],
        [rows_out, rows_out, line, line], rows_shape,
    )
    gain_sum = jnp.where(is_first, gain_0, gain_1)
    shift_sum = jnp.where(is_first, shift_0, shift_1)
    norms = small_exchange(
        jnp.concatenate([gain_sum, shift_sum], axis=0), ("dp", "tensor"), 4, True
    )

    blocks = micro * n_dp
    segment = jnp.swapaxes(all_segments, 0, 1).reshape(blocks, rows)
    all_tables, all_allowed = rotary_tables(segment), allowed_of(segment)
    column = lax.axis_index("dp") * (width // n_dp)
    slice_of = lambda x: lax.dynamic_slice_in_dim(x, column, width // n_dp, 1)
    inner = ((0,), (0,))

    def weight_terms(first, early, late, known, tables, allowed):
        normed_all, up_all = (early, late) if first else (late, early)
        *pieces, attended, s_q, s_v, s_up = attention_again(
            normed_all, up_all, proj_qkv, proj_dense, bias_qv, tables, allowed
        )
        activation, grad_pre, grad_fc_bias = hidden_call(
            first, late, known, fc_two if first else fc_one, bias_fc
        )
        normed_part, up_part = slice_of(normed_all), slice_of(up_all)
        return (
            jnp.stack([mm(normed_part, p, inner) for p in pieces]),
            mm(attended, up_part, inner),
            mm(normed_part, grad_pre, inner),
            mm(activation, up_part, inner),
            jnp.concatenate([s_q, s_v], axis=0),
            s_up[0],
            grad_fc_bias[0],
        )

    parts = -(-tokens // 4096)
    arrays = [early, late.reshape(tokens, width), known, all_tables, all_allowed]
    total = None
    for part in range(parts):
        pick = lambda x: x[part * x.shape[0] // parts : (part + 1) * x.shape[0] // parts]
        picked = [pick(x) for x in arrays]
        if total is not None:
            total, picked = settled((total, picked))
        terms = lax.cond(
            is_first,
            functools.partial(weight_terms, True),
            functools.partial(weight_terms, False),
            *picked,
        )
        total = terms if total is None else [x + y for x, y in zip(total, terms)]
    grad_qkv, grad_dense, grad_fc_one, grad_fc_two, grad_qv, grad_out, grad_fc_bias = total

    layer_out = jnp.where(is_first, out_0, out_1)
    in_grad = jnp.where(is_first, grad_0, grad_1)
    return (
        layer_out[None],
        in_grad[None],
        norms[:1],
        norms[1:],
        grad_qkv[None],
        grad_qv[None],
        grad_dense[None],
        grad_out[None],
        grad_fc_one[None],
        grad_fc_bias[None],
        grad_fc_two[None],
    )


def solution(mesh):
    return jax.shard_map(
        per_device,
        mesh=mesh,
        in_specs=(
            P(None, "dp", None),
            P(None, "dp", None),
            P(None, "dp"),
            P("section", None),
            P("section", None),
            P("section", None, None, "tensor"),
            P("section", None, "tensor"),
            P("section", "tensor", None),
            P("section", None),
            P("section", None, "tensor"),
            P("section", "tensor"),
            P("section", "tensor", None),
        ),
        out_specs=(
            P("section", None, ("dp", "tensor"), None),
            P("section", None, ("dp", "tensor"), None),
            P("section", None),
            P("section", None),
            P("section", None, "dp", "tensor"),
            P("section", None, "tensor"),
            P("section", "tensor", "dp"),
            P("section", None),
            P("section", "dp", "tensor"),
            P("section", "tensor"),
            P("section", "tensor", "dp"),
        ),
        check_vma=False,
    )
```

```python
import functools

import jax
import jax.numpy as jnp
from jax import lax
from jax.experimental import pallas as pl
from jax.experimental.pallas import tpu as pltpu
from jax.sharding import PartitionSpec as P

HEAD_DIM = 64
ROT = 32

NORM_EPS = 1e-05
MASKED = -1e30
MESH = pl.DeviceIdType.MESH


def rotary_tables(segment):
    blocks, length = segment.shape
    row_index = jnp.arange(length, dtype=jnp.int32)[None, :]
    previous = jnp.concatenate([segment[:, :1], segment[:, :-1]], axis=1)
    starts = jnp.where((row_index == 0) | (segment != previous), row_index, 0)
    position = (row_index - lax.cummax(starts, axis=1)).astype(jnp.float32)
    half_rot = ROT // 2
    frequency = 10000.0 ** (-2.0 * jnp.arange(half_rot, dtype=jnp.float32) / ROT)
    phase_angle = position[..., None] * frequency
    cos_part, sin_part = jnp.cos(phase_angle), jnp.sin(phase_angle)
    none = jnp.zeros((blocks, length, half_rot), jnp.float32)
    rest = jnp.ones((blocks, length, HEAD_DIM - ROT), jnp.float32)
    straight = jnp.concatenate([cos_part, cos_part, rest], axis=-1)
    from_upper = jnp.concatenate([-sin_part, none, 0.0 * rest], axis=-1)
    from_lower = jnp.concatenate([none, sin_part, 0.0 * rest], axis=-1)
    tables = jnp.stack([straight, from_upper, from_lower], axis=1)
    return jnp.concatenate([tables, tables], axis=-1)


def allowed_of(segment):
    length = segment.shape[-1]
    row_index = jnp.arange(length, dtype=jnp.int32)
    allowed = (segment[:, :, None] == segment[:, None, :]) & (
        row_index[None, :] <= row_index[:, None]
    )
    return allowed.astype(jnp.float32)


def mm(left, right, dims=((1,), (0,))):
    return lax.dot_general(left, right, (dims, ((), ())), preferred_element_type=jnp.float32)


def rotated(x, table, sign):
    half, lanes = ROT // 2, x.shape[-1]
    return (
        x * table[0]
        + pltpu.roll(x, lanes - half, 1) * (sign * table[1])
        + pltpu.roll(x, half, 1) * (sign * table[2])
    )


def softmax_of(query, key, allowed):
    scores = mm(query, key, ((1,), (1,))) * HEAD_DIM ** (-0.5)
    scores = jnp.where(allowed, scores, MASKED)
    exps = jnp.exp(scores - jnp.max(scores, axis=-1, keepdims=True))
    return exps * (1.0 / jnp.sum(exps, axis=-1, keepdims=True))


def stacked_heads(x):
    lane = lax.broadcasted_iota(jnp.int32, (1, x.shape[-1]), 1) // HEAD_DIM
    return jnp.concatenate(
        [
            x * jnp.where(lane == h, 1.0, 0.0).astype(x.dtype)
            for h in range(x.shape[-1] // HEAD_DIM)
        ],
        axis=0,
    )


def side_by_side(x, rows):
    lane = lax.broadcasted_iota(jnp.int32, (1, x.shape[-1]), 1) // HEAD_DIM
    out = x[:rows]
    for h in range(1, x.shape[0] // rows):
        out = jnp.where(lane == h, x[h * rows : (h + 1) * rows], out)
    return out


def attention_forward_kernel(qf_ref, kf_ref, vf_ref, table_ref, allowed_ref, q_ref, k_ref, v_ref, out_ref):
    bf16 = jnp.bfloat16
    table = table_ref[0]
    rows, lanes = table.shape[-2:]
    allowed = jnp.concatenate([allowed_ref[0] > 0.5] * (lanes // HEAD_DIM), axis=0)
    for pair in range(qf_ref.shape[-1] // lanes):
        at = slice(pair * lanes, (pair + 1) * lanes)
        query = rotated(qf_ref[:, at], table, 1.0).astype(bf16)
        key = rotated(kf_ref[:, at], table, 1.0).astype(bf16)
        value = vf_ref[:, at].astype(bf16)
        q_ref[:, at] = query
        k_ref[:, at] = key
        v_ref[:, at] = value
        prob = softmax_of(stacked_heads(query), key, allowed).astype(bf16)
        out_ref[:, at] = side_by_side(mm(prob, value), rows).astype(bf16)


def pair_backward(query, key, value, grad, table, allowed, with_output):
    bf16 = jnp.bfloat16
    rows, scale = query.shape[0], HEAD_DIM ** (-0.5)
    queries, grads = stacked_heads(query), stacked_heads(grad)
    prob_f = softmax_of(queries, key, allowed)
    prob_b = prob_f.astype(bf16)
    grad_prob = mm(grads, value, ((1,), (1,)))
    row_dot = jnp.sum(prob_f * grad_prob, axis=-1, keepdims=True)
    grad_score = (prob_f * (grad_prob - row_dot)).astype(bf16)
    g_query = side_by_side(mm(grad_score, key), rows)
    g_key = mm(grad_score, queries, ((0,), (0,)))
    g_value = mm(prob_b, grads, ((0,), (0,)))
    g_query = rotated(g_query * scale, table, -1.0)
    g_key = rotated(g_key * scale, table, -1.0)
    out = side_by_side(mm(prob_b, value), rows).astype(bf16) if with_output else None
    return g_query, g_key, g_value, out


def attention_backward_kernel(q_ref, k_ref, v_ref, ga_ref, table_ref, allowed_ref, gq_ref, gk_ref, gv_ref):
    bf16 = jnp.bfloat16
    table = table_ref[0]
    lanes = table.shape[-1]
    allowed = jnp.concatenate([allowed_ref[0] > 0.5] * (lanes // HEAD_DIM), axis=0)
    for pair in range(q_ref.shape[-1] // lanes):
        at = slice(pair * lanes, (pair + 1) * lanes)
        g_query, g_key, g_value, _ = pair_backward(
            q_ref[:, at], k_ref[:, at], v_ref[:, at], ga_ref[:, at], table, allowed, False
        )
        gq_ref[:, at] = g_query.astype(bf16)
        gk_ref[:, at] = g_key.astype(bf16)
        gv_ref[:, at] = g_value.astype(bf16)


def attention_again_kernel(
    normed_ref, up_ref, w_ref, dense_ref, bias_ref, table_ref, allowed_ref,
    gq_ref, gk_ref, gv_ref, out_ref, sq_ref, sv_ref, su_ref,
):
    bf16 = jnp.bfloat16
    count, _, rows, lanes = table_ref.shape
    features = gq_ref.shape[-1]
    wide = min(2 * lanes, features)

    @pl.when(pl.program_id(0) == 0)
    def _():
        sq_ref[...] = jnp.zeros_like(sq_ref)
        sv_ref[...] = jnp.zeros_like(sv_ref)
        su_ref[...] = jnp.zeros_like(su_ref)

    su_ref[...] += jnp.sum(up_ref[...].astype(jnp.float32), axis=0, keepdims=True)

    def products(at):
        cols = slice(at, at + wide)
        return (
            mm(normed_ref[...], w_ref[0, :, cols]) + bias_ref[0:1, cols],
            mm(normed_ref[...], w_ref[1, :, cols]),
            (mm(normed_ref[...], w_ref[2, :, cols]) + bias_ref[1:2, cols]).astype(bf16),
            mm(up_ref[...], dense_ref[cols, :], ((1,), (1,))).astype(bf16),
        )

    starts = list(range(0, features, wide))
    ready = products(starts[0])
    for index, start in enumerate(starts):
        upcoming = products(starts[index + 1]) if index + 1 < len(starts) else None
        for block in range(count):
            table = table_ref[block]
            allowed = jnp.concatenate([allowed_ref[block] > 0.5] * (lanes // HEAD_DIM), axis=0)
            down = slice(block * rows, (block + 1) * rows)
            for pair in range(wide // lanes):
                inside = slice(pair * lanes, (pair + 1) * lanes)
                query_f, key_f, value, grad = [x[down, inside] for x in ready]
                query = rotated(query_f, table, 1.0).astype(bf16)
                key = rotated(key_f, table, 1.0).astype(bf16)
                g_query, g_key, g_value, out = pair_backward(
                    query, key, value, grad, table, allowed, True
                )
                at = slice(start + pair * lanes, start + (pair + 1) * lanes)
                gq_ref[down, at] = g_query.astype(bf16)
                gk_ref[down, at] = g_key.astype(bf16)
                gv_ref[down, at] = g_value.astype(bf16)
                out_ref[down, at] = out
                sq_ref[:, at] += jnp.sum(g_query, axis=0, keepdims=True)
                sv_ref[:, at] += jnp.sum(g_value, axis=0, keepdims=True)
        ready = upcoming


def attention_again(normed, up, proj_qkv, proj_dense, bias_qv, tables, allowed):
    blocks, _, rows, lanes = tables.shape
    features, width = proj_dense.shape
    count = 2 if blocks % 2 == 0 else 1
    wide = pl.BlockSpec((count * rows, width), lambda i: (i, 0))
    block = pl.BlockSpec((count * rows, features), lambda i: (i, 0))
    one = pl.BlockSpec((1, features), lambda i: (0, 0))
    flat = jax.ShapeDtypeStruct((blocks * rows, features), jnp.bfloat16)
    line = jax.ShapeDtypeStruct((1, features), jnp.float32)
    once = pl.Buffered(1)
    return pl.pallas_call(
        attention_again_kernel,
        grid=(blocks // count,),
        in_specs=[
            wide,
            wide,
            pl.BlockSpec(proj_qkv.shape, lambda i: (0, 0, 0), pipeline_mode=once),
            pl.BlockSpec(proj_dense.shape, lambda i: (0, 0), pipeline_mode=once),
            pl.BlockSpec(bias_qv.shape, lambda i: (0, 0)),
            pl.BlockSpec((count, 3, rows, lanes), lambda i: (i, 0, 0, 0)),
            pl.BlockSpec((count, rows, rows), lambda i: (i, 0, 0)),
        ],
        out_specs=[block] * 4 + [one] * 2 + [pl.BlockSpec((1, width), lambda i: (0, 0))],
        out_shape=[flat] * 4 + [line] * 2 + [jax.ShapeDtypeStruct((1, width), jnp.float32)],
        cost_estimate=pl.CostEstimate(
            flops=8 * blocks * rows * width * features,
            bytes_accessed=blocks * rows * (width * 4 + features * 8),
            transcendentals=0,
        ),
    )(normed, up, proj_qkv, proj_dense, bias_qv, tables, allowed)


def attention_call(kernel, arrays, tables, allowed, outs):
    blocks, _, rows, lanes = tables.shape
    features = arrays[0].shape[-1]
    block = pl.BlockSpec((rows, features), lambda i: (i, 0))
    flat = (blocks * rows, features)
    return pl.pallas_call(
        kernel,
        grid=(blocks,),
        in_specs=[block] * len(arrays)
        + [
            pl.BlockSpec((1, 3, rows, lanes), lambda i: (i, 0, 0, 0)),
            pl.BlockSpec((1, rows, rows), lambda i: (i, 0, 0)),
        ],
        out_specs=[block] * outs,
        out_shape=[jax.ShapeDtypeStruct(flat, jnp.bfloat16)] * outs,
        cost_estimate=pl.CostEstimate(
            flops=20 * blocks * rows * rows * features,
            bytes_accessed=blocks * rows * features * 16,
            transcendentals=0,
        ),
    )(*arrays, tables, allowed)


def projections(normed, proj_qkv, bias_qv):
    return [
        mm(normed, proj_qkv[0]) + bias_qv[0],
        mm(normed, proj_qkv[1]),
        mm(normed, proj_qkv[2]) + bias_qv[1],
    ]


def settled(x):
    return lax.optimization_barrier(x)


def gelu_grad(pre_act, grad_act):
    _, pull_back = jax.vjp(lambda value_in: jax.nn.gelu(value_in, approximate=True), pre_act)
    return pull_back(grad_act)[0]


def normalize(hidden, norm_gain, norm_shift):
    residual = hidden.astype(jnp.float32)
    centred = residual - jnp.mean(residual, axis=-1, keepdims=True)
    inv_std = lax.rsqrt(jnp.mean(centred * centred, axis=-1, keepdims=True) + NORM_EPS)
    return (centred * inv_std * norm_gain + norm_shift).astype(jnp.bfloat16)


def partner(t, k):
    out, bit = t, 1
    while bit <= k:
        if k & bit:
            out = out + (1 - 2 * (lax.rem(lax.div(t, bit), 2))) * bit
        bit *= 2
    return out


def enter(n):
    t, sec = lax.axis_index("tensor"), lax.axis_index("section")
    barrier = pltpu.get_barrier_semaphore()
    for k in range(1, n):
        pl.semaphore_signal(
            barrier, inc=1, device_id={"tensor": partner(t, k)}, device_id_type=MESH
        )
    pl.semaphore_signal(barrier, inc=1, device_id={"section": 1 - sec}, device_id_type=MESH)
    pl.semaphore_wait(barrier, n)


def send(src, dst, sems, device):
    copy = pltpu.make_async_remote_copy(
        src_ref=src, dst_ref=dst, send_sem=sems[0], recv_sem=sems[1],
        device_id=device, device_id_type=MESH,
    )
    copy.start()
    return copy


def halves_of(width):
    sec = lax.axis_index("section")
    half = width // 2
    return (
        pl.ds(pl.multiple_of(sec * half, half), half),
        pl.ds(pl.multiple_of((1 - sec) * half, half), half),
    )


def start_swaps(n, partial_ref, scratch):
    pair, _, _, pair_sems, _ = scratch
    t, sec = lax.axis_index("tensor"), lax.axis_index("section")
    _, other = halves_of(partial_ref.shape[-1])
    return {
        k: send(
            partial_ref.at[:, partner(t, k), :, other], pair.at[k],
            [x.at[k] for x in pair_sems], {"section": 1 - sec},
        )
        for k in range(n - 1, -1, -1)
    }


def start_sums(n, partial_ref, scratch, swaps):
    pair, out_buf, recv, _, rs_sems = scratch
    t = lax.axis_index("tensor")
    mine, _ = halves_of(partial_ref.shape[-1])
    sends = []
    for k in range(n - 1, -1, -1):
        at = partner(t, k)
        swaps[k].wait_recv()
        both = partial_ref[:, at, :, mine].astype(jnp.float32) + pair[k].astype(jnp.float32)
        if k:
            out_buf[k - 1] = both.astype(jnp.bfloat16)
            sends.append(
                (k, send(out_buf.at[k - 1], recv.at[k - 1],
                         [x.at[k - 1] for x in rs_sems], {"tensor": at}))
            )
    return both, sends


def finish_sums(total, scratch, sends):
    recv = scratch[2]
    for k, copy in sends:
        copy.wait_recv()
        total = total + recv[k - 1].astype(jnp.float32)
    return total


def reduced_half(n, partial_ref, scratch):
    enter(n)
    swaps = start_swaps(n, partial_ref, scratch)
    total, sends = start_sums(n, partial_ref, scratch, swaps)
    total = finish_sums(total, scratch, sends)
    return total, list(swaps.values()) + [copy for _, copy in sends]


def spread(n, full_ref, ag_sems, fw_sems):
    t, sec = lax.axis_index("tensor"), lax.axis_index("section")
    mine, _ = halves_of(full_ref.shape[-1])
    own = full_ref.at[:, t, :, mine]
    copies = [
        send(own, own, [x.at[k - 1] for x in ag_sems], {"tensor": partner(t, k)})
        for k in range(n - 1, 0, -1)
    ]
    passed = []
    for k, copy in zip(range(n - 1, 0, -1), copies):
        copy.wait_recv()
        part = full_ref.at[:, partner(t, k), :, mine]
        passed.append(send(part, part, [x.at[k - 1] for x in fw_sems], {"section": 1 - sec}))
    for copy in copies:
        copy.wait_send()
    for copy in passed:
        copy.wait()


def standard_of(rows):
    centred = rows - jnp.mean(rows, axis=-1, keepdims=True)
    inv_std = lax.rsqrt(jnp.mean(centred * centred, axis=-1, keepdims=True) + NORM_EPS)
    return centred * inv_std, inv_std


def forward_kernel(
    n, partial_ref, resid_ref, bias_ref, gain_ref, shift_ref, out_ref, full_ref, *scratch
):
    t, sec = lax.axis_index("tensor"), lax.axis_index("section")
    mine, _ = halves_of(partial_ref.shape[-1])
    total, copies = reduced_half(n, partial_ref, unpack(scratch))
    total = total + resid_ref[:, :, mine].astype(jnp.float32) + bias_ref[:, mine][None]
    out_ref[:, :, mine] = total.astype(jnp.bfloat16)
    part = out_ref.at[:, :, mine]
    hop = send(part, part, scratch[7:9], {"section": 1 - sec})
    hop.wait()
    standard, _ = standard_of(out_ref[...].astype(jnp.float32))
    full_ref[:, t] = (standard * gain_ref[...][None] + shift_ref[...][None]).astype(jnp.bfloat16)
    spread(n, full_ref, scratch[9:11], scratch[11:13])
    for copy in copies:
        copy.wait_send()


def unpack(scratch):
    pair, out_buf, recv, pair_s, pair_r, rs_s, rs_r = scratch[:7]
    return pair, out_buf, recv, (pair_s, pair_r), (rs_s, rs_r)


def norm_backward(grad_normed, hidden_ref, gain_ref, up_rows, ggain_ref, gshift_ref):
    standard, inv_std = standard_of(hidden_ref[...].astype(jnp.float32))
    scaled = grad_normed * gain_ref[...][None]
    grad_in = inv_std * (
        scaled
        - jnp.mean(scaled, axis=-1, keepdims=True)
        - standard * jnp.mean(scaled * standard, axis=-1, keepdims=True)
    )
    ggain_ref[...] = jnp.sum(jnp.sum(grad_normed * standard, axis=0), axis=0, keepdims=True)
    gshift_ref[...] = jnp.sum(jnp.sum(grad_normed, axis=0), axis=0, keepdims=True)
    return (up_rows.astype(jnp.float32) + grad_in).astype(jnp.bfloat16)


def backward_kernel(
    n, partial_ref, up_ref, hidden_ref, gain_ref, out_ref, ggain_ref, gshift_ref, full_ref,
    whole, *scratch
):
    t, sec = lax.axis_index("tensor"), lax.axis_index("section")
    mine, _ = halves_of(partial_ref.shape[-1])
    total, copies = reduced_half(n, partial_ref, unpack(scratch))
    whole[:, :, mine] = total
    part = whole.at[:, :, mine]
    hop = send(part, part, scratch[7:9], {"section": 1 - sec})
    hop.wait()
    out_ref[...] = norm_backward(
        whole[...], hidden_ref, gain_ref, up_ref[:, t], ggain_ref, gshift_ref
    )
    full_ref[:, t] = out_ref[...]
    spread(n, full_ref, scratch[9:11], scratch[11:13])
    for copy in copies:
        copy.wait_send()


def final_kernel(
    n, partial_ref, resid_ref, bias_ref, grad_ref, up_ref, hidden_ref, gain_ref,
    out_ref, down_ref, ggain_ref, gshift_ref, whole, *scratch
):
    t, sec = lax.axis_index("tensor"), lax.axis_index("section")
    mine, _ = halves_of(partial_ref.shape[-1])
    sets = [unpack(scratch[:9]), unpack(scratch[9:])]
    hops = [scratch[7:9], scratch[16:18]]
    refs = [grad_ref, partial_ref]
    enter(n)
    swaps = [start_swaps(n, ref, x) for ref, x in zip(refs, sets)]
    sums = [start_sums(n, ref, x, w) for ref, x, w in zip(refs, sets, swaps)]
    whole[:, :, mine] = finish_sums(sums[0][0], sets[0], sums[0][1])
    part = whole.at[:, :, mine]
    first = send(part, part, hops[0], {"section": 1 - sec})
    total = finish_sums(sums[1][0], sets[1], sums[1][1])
    total = total + resid_ref[:, :, mine].astype(jnp.float32) + bias_ref[:, mine][None]
    out_ref[:, :, mine] = total.astype(jnp.bfloat16)
    part = out_ref.at[:, :, mine]
    second = send(part, part, hops[1], {"section": 1 - sec})
    first.wait()
    down_ref[...] = norm_backward(
        whole[...], hidden_ref, gain_ref, up_ref[:, t], ggain_ref, gshift_ref
    )
    second.wait()
    for w in swaps:
        for copy in w.values():
            copy.wait_send()
    for _, sends in sums:
        for _, copy in sends:
            copy.wait_send()


def sum_call(kernel, n, ident, args, outs, rows_shape):
    dma = pltpu.SemaphoreType.DMA
    half = rows_shape[:-1] + (rows_shape[-1] // 2,)
    scratch = [
        pltpu.VMEM((n,) + half, jnp.bfloat16),
        pltpu.VMEM((n - 1,) + half, jnp.bfloat16),
        pltpu.VMEM((n - 1,) + half, jnp.bfloat16),
        dma((n,)), dma((n,)), dma((n - 1,)), dma((n - 1,)), dma, dma,
    ]
    scratch += scratch if kernel is final_kernel else [dma((n - 1,))] * 4
    if kernel is not forward_kernel:
        scratch = [pltpu.VMEM(rows_shape, jnp.float32)] + scratch
    vmem = pl.BlockSpec(memory_space=pltpu.VMEM)
    return pl.pallas_call(
        functools.partial(kernel, n),
        out_shape=outs,
        in_specs=[vmem] * len(args),
        out_specs=[vmem] * len(outs),
        scratch_shapes=scratch,
        compiler_params=pltpu.CompilerParams(
            collective_id=ident, has_side_effects=True, vmem_limit_bytes=32 * 1024 * 1024
        ),
    )(*args)


GELU_A = (2.0 / jnp.pi) ** 0.5
GELU_B = 0.044715


def hidden_kernel(first, x_ref, known_ref, w_ref, b_ref, act_ref, grad_ref, sum_ref):
    @pl.when(pl.program_id(1) == 0)
    def _():
        sum_ref[...] = jnp.zeros_like(sum_ref)

    step = 256
    starts = list(range(0, act_ref.shape[-1], step))

    def product(at):
        cols = slice(at, at + step)
        if first:
            return mm(x_ref[...], w_ref[cols, :], ((1,), (1,)))
        return mm(x_ref[...], w_ref[:, cols]) + b_ref[:, cols]

    ready = product(starts[0])
    for index, at in enumerate(starts):
        cols = slice(at, at + step)
        upcoming = product(starts[index + 1]) if index + 1 < len(starts) else None
        pre, grad_act = (known_ref[:, cols], ready) if first else (ready, known_ref[:, cols])
        square = pre * pre
        bent = jnp.tanh(pre * (GELU_A + (GELU_A * GELU_B) * square))
        gate = 0.5 + 0.5 * bent
        act_ref[:, cols] = (pre * gate).astype(jnp.bfloat16)
        slope = gate + (0.5 * pre) * (1.0 - bent * bent) * (
            GELU_A + (3.0 * GELU_A * GELU_B) * square
        )
        grad_pre = grad_act * slope
        grad_ref[:, cols] = grad_pre.astype(jnp.bfloat16)
        sum_ref[:, cols] += jnp.sum(grad_pre, axis=0, keepdims=True)
        ready = upcoming


def hidden_call(first, x, known, weight, bias):
    tokens, width = x.shape
    units = known.shape[-1]
    tile, chunk = 512 if tokens % 512 == 0 else 256, min(1024, units)
    flat = pl.BlockSpec((tile, chunk), lambda j, i: (i, j))
    line = pl.BlockSpec((1, chunk), lambda j, i: (0, j))
    w_spec = (
        pl.BlockSpec((chunk, width), lambda j, i: (j, 0))
        if first
        else pl.BlockSpec((width, chunk), lambda j, i: (0, j))
    )
    out = jax.ShapeDtypeStruct((tokens, units), jnp.bfloat16)
    return pl.pallas_call(
        functools.partial(hidden_kernel, first),
        grid=(units // chunk, tokens // tile),
        in_specs=[pl.BlockSpec((tile, width), lambda j, i: (i, 0)), flat, w_spec, line],
        out_specs=[flat, flat, line],
        out_shape=[out, out, jax.ShapeDtypeStruct((1, units), jnp.float32)],
        cost_estimate=pl.CostEstimate(
            flops=2 * tokens * width * units,
            bytes_accessed=tokens * (units * 8 + width * 4),
            transcendentals=tokens * units,
        ),
    )(x, known, weight, bias[None])


def exchange_kernel(axes, add, x_ref, out_ref, *rest):
    gathered, send_sem, recv_sem = rest if add else (out_ref,) + rest
    sizes = [lax.axis_size(a) for a in axes]
    index = [lax.axis_index(a) for a in axes]
    count = 1
    mine = 0
    for s, i in zip(sizes, index):
        count *= s
        mine = mine * s + i

    def shifted(k):
        ids = {}
        for a, s, i in zip(reversed(axes), reversed(sizes), reversed(index)):
            ids[a] = lax.rem(i + k % s, s)
            k //= s
        return ids

    barrier = pltpu.get_barrier_semaphore()
    for k in range(1, count):
        pl.semaphore_signal(barrier, inc=1, device_id=shifted(k), device_id_type=MESH)
    pl.semaphore_wait(barrier, count - 1)
    copies = []
    for k in range(1, count):
        copy = pltpu.make_async_remote_copy(
            src_ref=x_ref,
            dst_ref=gathered.at[mine],
            send_sem=send_sem.at[k],
            recv_sem=recv_sem.at[k],
            device_id=shifted(k),
            device_id_type=MESH,
        )
        copy.start()
        copies.append(copy)
    gathered[mine] = x_ref[...]
    for copy in copies:
        copy.wait()
    if add:
        total = gathered[0]
        for i in range(1, count):
            total = total + gathered[i]
        out_ref[...] = total


def small_exchange(x, axes, ident, add):
    count = 1
    for a in axes:
        count *= lax.axis_size(a)
    vmem = pl.BlockSpec(memory_space=pltpu.VMEM)
    stacked = (count,) + x.shape
    return pl.pallas_call(
        functools.partial(exchange_kernel, axes, add),
        out_shape=jax.ShapeDtypeStruct(x.shape if add else stacked, x.dtype),
        in_specs=[vmem],
        out_specs=vmem,
        scratch_shapes=([pltpu.VMEM(stacked, x.dtype)] if add else [])
        + [pltpu.SemaphoreType.DMA((count,)), pltpu.SemaphoreType.DMA((count,))],
        compiler_params=pltpu.CompilerParams(collective_id=ident, has_side_effects=True),
    )(x)


def per_device(
    block_input,
    cotangent,
    segments,
    ln_gain,
    ln_bias,
    qkv_weight,
    qv_bias,
    dense_weight,
    out_bias,
    fc1_weight,
    fc1_bias,
    fc2_weight,
):
    micro, rows, width = block_input.shape
    n = lax.axis_size("tensor")
    n_dp = lax.axis_size("dp")
    share = rows // n
    sec = lax.axis_index("section")
    is_first = sec == 0
    row_start = lax.axis_index("tensor") * share
    proj_qkv, proj_dense, fc_one, fc_two = (
        qkv_weight[0], dense_weight[0], fc1_weight[0], fc2_weight[0]
    )
    bias_qv, bias_fc = qv_bias[0], fc1_bias[0]
    bf16, f32 = jnp.bfloat16, jnp.float32
    features, hidden_units = proj_qkv.shape[-1], fc_one.shape[-1]

    swap = lambda x: lax.ppermute(x, "section", [(0, 1), (1, 0)])

    def half(x, axis, which):
        size = x.shape[axis] // 2
        return lax.dynamic_slice_in_dim(x, which * size, size, axis)

    def both(x, axis):
        return half(x, axis, sec), swap(half(x, axis, 1 - sec))

    def of_layer(index, pair):
        return jnp.where(sec == index, pair[0], pair[1])

    small = jnp.concatenate(
        [ln_gain[0], ln_bias[0], out_bias[0], bias_qv.reshape(-1), bias_fc]
    )[None]
    small_pair = (small, swap(small))
    weight_pairs = [
        both(proj_qkv, 2), both(fc_one, 1), both(proj_dense, 0), both(fc_two, 0)
    ]

    def parameters(index):
        vector = of_layer(index, small_pair)[0]
        gain, shift, bias = [vector[None, i * width : (i + 1) * width] for i in range(3)]
        at = 3 * width
        b_qv = half(vector[at : at + 2 * features].reshape(2, features), 1, sec)
        b_fc = half(vector[at + 2 * features :], 0, sec)
        return gain, shift, bias, b_qv, b_fc, [of_layer(index, p) for p in weight_pairs]

    layers = [parameters(0), parameters(1)]

    live = (segments >= 0)[:, :, None].astype(bf16)
    top = cotangent * live
    own_rows = lambda x: lax.dynamic_slice_in_dim(x, row_start, share, 1)
    first_normed = normalize(block_input, layers[0][0], layers[0][1])
    x_rows = own_rows(block_input)
    all_segments = small_exchange(segments, ("dp",), 5, False)
    tables, allowed = rotary_tables(segments), allowed_of(segments)

    def gather(x):
        return lax.all_gather(x, ("dp", "tensor"), axis=1, tiled=True)

    early = lax.all_gather(
        jnp.where(is_first, first_normed, top), "dp", axis=1, tiled=True
    )

    four = lambda x: x.reshape(micro, n, share, width)
    flat = lambda x: x.reshape(micro * rows, width)
    sds = jax.ShapeDtypeStruct
    rows_shape = (micro, share, width)
    rows_out, full_out = sds(rows_shape, bf16), sds((micro, n, share, width), bf16)
    line = sds((1, width), f32)

    def branch_forward(normed, layer):
        _, _, _, b_qv, b_fc, (w_qkv, w_one, w_dense, w_two) = layer
        *kept, attended = attention_call(
            attention_forward_kernel, projections(normed, w_qkv, b_qv), tables, allowed, 4,
        )
        pre_act = mm(normed, w_one) + b_fc
        activation = settled(jax.nn.gelu(pre_act, approximate=True).astype(bf16))
        partial = (mm(attended, w_dense) + mm(activation, w_two)).astype(bf16)
        return four(partial), (kept, pre_act)

    def branch_backward(up, layer, stored):
        kept, pre_act = stored
        w_qkv, w_one, w_dense, w_two = layer[-1]
        grad_pre = settled(gelu_grad(pre_act, mm(up, w_two, ((1,), (1,)))).astype(bf16))
        grad_att = mm(up, w_dense, ((1,), (1,))).astype(bf16)
        pieces = attention_call(
            attention_backward_kernel, kept + [grad_att], tables, allowed, 3,
        )
        grad_normed = mm(grad_pre, w_one, ((1,), (1,)))
        for which in range(3):
            grad_normed = grad_normed + mm(pieces[which], w_qkv[which], ((1,), (1,)))
        return four(grad_normed.astype(bf16))

    partial, stored_0 = branch_forward(flat(first_normed), layers[0])
    out_0, normed = sum_call(
        forward_kernel, n, 0,
        [partial, x_rows, layers[0][2], layers[1][0], layers[1][1]],
        [rows_out, full_out], rows_shape,
    )
    last_partial, stored_1 = branch_forward(flat(normed), layers[1])
    partial = branch_backward(flat(top), layers[1], stored_1)
    grad_1, gain_1, shift_1, up = sum_call(
        backward_kernel, n, 2, [partial, four(top), out_0, layers[1][0]],
        [rows_out, line, line, full_out], rows_shape,
    )
    own = lambda x: lax.dynamic_index_in_dim(x, lax.axis_index("tensor"), 1, keepdims=False)
    late_rows = jnp.where(is_first, grad_1, own(normed))
    up, late_rows, early = settled((up, late_rows, early))
    late = gather(late_rows)
    partial = branch_backward(flat(up), layers[0], stored_0)

    tokens = micro * n_dp * rows
    early = early.reshape(tokens, width)
    known = lax.cond(
        is_first,
        lambda x: mm(x, fc_one) + bias_fc,
        lambda x: mm(x, fc_two, ((1,), (1,))),
        early,
    )
    partial, last_partial, known = settled((partial, last_partial, known))
    out_1, grad_0, gain_0, shift_0 = sum_call(
        final_kernel, n, 1,
        [last_partial, out_0, layers[1][2], partial, up, x_rows, layers[0][0]],
        [rows_out, rows_out, line, line], rows_shape,
    )
    gain_sum = jnp.where(is_first, gain_0, gain_1)
    shift_sum = jnp.where(is_first, shift_0, shift_1)
    norms = small_exchange(
        jnp.concatenate([gain_sum, shift_sum], axis=0), ("dp", "tensor"), 4, True
    )

    blocks = micro * n_dp
    segment = jnp.swapaxes(all_segments, 0, 1).reshape(blocks, rows)
    all_tables, all_allowed = rotary_tables(segment), allowed_of(segment)
    column = lax.axis_index("dp") * (width // n_dp)
    slice_of = lambda x: lax.dynamic_slice_in_dim(x, column, width // n_dp, 1)
    inner = ((0,), (0,))

    def weight_terms(first, early, late, known, tables, allowed):
        normed_all, up_all = (early, late) if first else (late, early)
        *pieces, attended, s_q, s_v, s_up = attention_again(
            normed_all, up_all, proj_qkv, proj_dense, bias_qv, tables, allowed
        )
        activation, grad_pre, grad_fc_bias = hidden_call(
            first, late, known, fc_two if first else fc_one, bias_fc
        )
        normed_part, up_part = slice_of(normed_all), slice_of(up_all)
        return (
            jnp.stack([mm(normed_part, p, inner) for p in pieces]),
            mm(attended, up_part, inner),
            mm(normed_part, grad_pre, inner),
            mm(activation, up_part, inner),
            jnp.concatenate([s_q, s_v], axis=0),
            s_up[0],
            grad_fc_bias[0],
        )

    parts = -(-tokens // 4096)
    arrays = [early, late.reshape(tokens, width), known, all_tables, all_allowed]
    total = None
    for part in range(parts):
        pick = lambda x: x[part * x.shape[0] // parts : (part + 1) * x.shape[0] // parts]
        picked = [pick(x) for x in arrays]
        if total is not None:
            total, picked = settled((total, picked))
        terms = lax.cond(
            is_first,
            functools.partial(weight_terms, True),
            functools.partial(weight_terms, False),
            *picked,
        )
        total = terms if total is None else [x + y for x, y in zip(total, terms)]
    grad_qkv, grad_dense, grad_fc_one, grad_fc_two, grad_qv, grad_out, grad_fc_bias = total

    layer_out = jnp.where(is_first, out_0, out_1)
    in_grad = jnp.where(is_first, grad_0, grad_1)
    return (
        layer_out[None],
        in_grad[None],
        norms[:1],
        norms[1:],
        grad_qkv[None],
        grad_qv[None],
        grad_dense[None],
        grad_out[None],
        grad_fc_one[None],
        grad_fc_bias[None],
        grad_fc_two[None],
    )


def solution(mesh):
    return jax.shard_map(
        per_device,
        mesh=mesh,
        in_specs=(
            P(None, "dp", None),
            P(None, "dp", None),
            P(None, "dp"),
            P("section", None),
            P("section", None),
            P("section", None, None, "tensor"),
            P("section", None, "tensor"),
            P("section", "tensor", None),
            P("section", None),
            P("section", None, "tensor"),
            P("section", "tensor"),
            P("section", "tensor", None),
        ),
        out_specs=(
            P("section", None, ("dp", "tensor"), None),
            P("section", None, ("dp", "tensor"), None),
            P("section", None),
            P("section", None),
            P("section", None, "dp", "tensor"),
            P("section", None, "tensor"),
            P("section", "tensor", "dp"),
            P("section", None),
            P("section", "dp", "tensor"),
            P("section", "tensor"),
            P("section", "tensor", "dp"),
        ),
        check_vma=False,
    )
```
